512 devices in a mesh: group: 2 (over y), seq: 128 (over x, z), head: 2 (over core).
Axes of the slice: x: 4, y: 2, z: 32, core: 2. Of those that a mesh axis runs over, the one named last changes fastest.
The devices are a block of a 4x8x32 slice.
Arguments:
- queries: bfloat16 [32768, 3, 2560], P(('group', 'seq'), None, 'head'), parts along dimension 0, may hold values from -6 to 6, as said below
- keys: bfloat16 [32768, 512], P(('group', 'seq'), 'head'), parts along dimension 0, may hold values from -6 to 6, as said below
- values: bfloat16 [32768, 512], P(('group', 'seq'), 'head'), parts along dimension 0, may hold values from -6 to 6
- lengths: int32 [128], P('group'), parts along dimension 0, may hold values from 1 to 1024, 16384 in all
- page_owner: int32 [8192, 4], P(('group', 'seq'), 'head'), parts along dimension 0, may hold values from 0 to 127, as said below
- page_slot: int32 [8192, 4], P(('group', 'seq'), 'head'), parts along dimension 0, may hold values from 0 to 63, as said below
Outputs:
- attended: bfloat16 [32768, 3, 2560], P(('group', 'seq'), None, 'head'), parts along dimension 0
- cache_pages: bfloat16 [32768, 4, 256], P(('group', 'seq', 'head')), parts along dimension 0
The draws below stay inside these ranges and needn't reach their ends.
There are 2 independent parts, one for each index of `group`. The reference program is written for one: setup_inputs(seed, part) draws one part's arguments, and reference() takes and returns one part's arrays. A program takes and returns all parts, laid end to end along the dimension named above; each array names one. Nothing has to cross between parts.
Inputs may be any that keep to these rules, and one draw needn't show every extreme that they name: `page_owner`: for each index g of the head axis, the pages of KV heads g * 2 to g * 2 + 1 held by one index of seq include at most one page for any one owner, and that bound is reached; every owner receives exactly 64 such pages. `page_slot`: the pages that one owner receives for one index of the head axis have distinct slots. `queries`: entries lie within the range; they are of order one. `keys`: entries lie within the range; they are of order one. `lengths`: sum to 16384; the largest is exactly 1024.
All inputs are finite; a program needn't handle non-finite values.
Results may differ from the reference program's by a relative error of at most 0.0029.
Values may be sent and summed in bfloat16 or wider, within the bound.
A program may use at most 64 MiB of HBM per device.

```python
import math
import jax
import jax.numpy as jnp
import numpy as np
from jax import lax

TOK_DEV = 128
LAYERS = 3
KV_HEADS = 4
QPER = 5
HD = 128
PAGE = 4
Q_HEADS = 20
MAXLEN = 1024
REQS = 64
TOKENS = 16384
PAGES = 4096
PAGES_DEV = 32
KV_LOCAL = 2
SLOTS = 64
N_SEQ = 128
N_HEAD = 2


def draw_keys(key, part):
    shape = (TOKENS, KV_HEADS * HD)
    drawn = 1.4 * jax.random.normal(jax.random.fold_in(key, 3), shape, jnp.float32)
    return jnp.clip(drawn, -6.0, 6.0).astype(jnp.bfloat16)


def draw_queries(key, part):
    shape = (TOKENS, LAYERS, Q_HEADS * HD)
    drawn = 1.4 * jax.random.normal(jax.random.fold_in(key, 5), shape, jnp.float32)
    return jnp.clip(drawn, -6.0, 6.0).astype(jnp.bfloat16)


def page_plan(key):
    base = jax.random.fold_in(key, 4242)
    owners = []
    slots = []
    for group in range(N_HEAD):
        group_key = jax.random.fold_in(base, group)
        sigma = jax.random.permutation(jax.random.fold_in(group_key, 1), N_SEQ).astype(jnp.int32)
        tau = jax.random.permutation(jax.random.fold_in(group_key, 2), N_SEQ).astype(jnp.int32)
        offsets = jax.random.permutation(jax.random.fold_in(group_key, 3), max(SLOTS, N_SEQ))[:SLOTS].astype(jnp.int32) % N_SEQ
        row_keys = jax.random.split(jax.random.fold_in(group_key, 4), N_SEQ)
        orders = jax.vmap(lambda subkey: jax.random.permutation(subkey, SLOTS))(row_keys).astype(jnp.int32)
        pages = jnp.arange(PAGES, dtype=jnp.int32)
        source = pages // PAGES_DEV
        within = pages % PAGES_DEV
        local = jnp.arange(KV_LOCAL, dtype=jnp.int32)
        number = within[:, None] * KV_LOCAL + local[None, :]
        owner = sigma[(tau[source][:, None] + offsets[number]) % N_SEQ]
        owners.append(owner)
        slots.append(orders[owner, number])
    return (jnp.concatenate(owners, axis=1).astype(jnp.int32), jnp.concatenate(slots, axis=1).astype(jnp.int32))


def draw_page_owner(key, part):
    return page_plan(key)[0]


def draw_page_slot(key, part):
    return page_plan(key)[1]


def shard_levels(own_key, extent, cuts, smallest, high):
    level = 1.0
    for position, blocks in cuts:
        steps = jax.random.uniform(jax.random.fold_in(jax.random.fold_in(own_key, 6), position), (blocks,), jnp.float32, smallest / len(cuts), high / len(cuts))
        level = level * jnp.repeat(jnp.exp(steps), extent[position] // blocks).reshape((-1,) + (1,) * (len(extent) - 1 - position))
    return level


def split_up(number_of, total, reach, slope):
    portions = [(1 << 20) // math.isqrt(grade ** slope) + 1 for grade in range(2, number_of + 1)]
    rest, counts = total - reach - (number_of - 1), [1] * (number_of - 1)
    while rest > 0:
        movable = [i for i in range(number_of - 1) if counts[i] < reach]
        whole, left = sum([portions[i] for i in movable]), rest
        for i in movable:
            addition = min(reach - counts[i], max(1, left * portions[i] // whole), rest)
            counts[i] = counts[i] + addition
            rest = rest - addition
    return np.array([reach] + counts)


def uneven_parts(key, amount, total, most, lean):
    if amount == 2:
        one = jax.random.randint(key, (), max(1, total - most), min(most, total - 1) + 1)
        return jnp.stack([one, total - one])
    sizes = jnp.asarray(split_up(amount, total, most, lean), jnp.int32)
    couples = (amount - 1) // 2
    donor, receiver = sizes[1:1 + 2 * couples:2], sizes[2:2 + 2 * couples:2]
    margin = jnp.minimum(donor - 1, most - receiver)
    shifted = jax.random.randint(jax.random.fold_in(key, 1), (couples,), 0, 1 << 20) % (margin + 1)
    sizes = sizes.at[1:1 + 2 * couples:2].set(donor - shifted).at[2:2 + 2 * couples:2].set(receiver + shifted)
    return sizes[jax.random.permutation(jax.random.fold_in(key, 2), amount)]


def gaussian(own_key, extent, scale, limit, shards=(), kind=jnp.bfloat16):
    entries = jax.random.normal(own_key, extent, jnp.float32) * scale
    if len(shards) > 0:
        entries = shard_levels(own_key, extent, shards, -0.22, 0.18) * entries
    return jnp.clip(entries, min=-limit, max=limit).astype(kind)


def setup_inputs(seed: int = 0, part: int = 0) -> dict:
    splits = jax.random.split(jax.random.key(seed), 7)
    own_keys = jax.random.split(jax.random.fold_in(splits[6], part), 7)
    return {
        "queries": draw_queries(jax.random.fold_in(jax.random.fold_in(splits[6], part), 71), part),
        "keys": draw_keys(jax.random.fold_in(jax.random.fold_in(splits[6], part), 71), part),
        "values": gaussian(own_keys[2], (TOKENS, KV_HEADS * HD), 1.0, 6.0, ((0, 128), (1, 2))),
        "lengths": uneven_parts(own_keys[3], REQS, TOKENS, MAXLEN, 2).astype(jnp.int32),
        "page_owner": draw_page_owner(jax.random.fold_in(jax.random.fold_in(splits[6], part), 71), part),
        "page_slot": draw_page_slot(jax.random.fold_in(jax.random.fold_in(splits[6], part), 71), part),
    }


def reference(queries, keys, values, lengths, page_owner, page_slot):
    starts = jnp.cumsum(lengths) - lengths
    positions = jnp.arange(TOKENS, dtype=jnp.int32)
    requests = lax.optimization_barrier(jnp.sum((starts[None, :] <= positions[:, None]).astype(jnp.int32), axis=1)) - 1
    lead = MAXLEN
    width = lead + TOK_DEV
    keys_pad = jnp.concatenate([jnp.zeros((lead, KV_HEADS * HD), keys.dtype), keys], axis=0)
    vals_pad = jnp.concatenate([jnp.zeros((lead, KV_HEADS * HD), values.dtype), values], axis=0)
    req_pad = jnp.concatenate([jnp.full((lead,), -1, jnp.int32), requests.astype(jnp.int32)], axis=0)
    scale = 1.0 / math.sqrt(HD)

    def one_block(index):
        begin = (index * TOK_DEV).astype(jnp.int32)
        query_block = lax.dynamic_slice_in_dim(queries, begin, TOK_DEV, 0).astype(jnp.float32)
        query_block = query_block.reshape(TOK_DEV, LAYERS, KV_HEADS, QPER, HD)
        key_block = lax.dynamic_slice_in_dim(keys_pad, begin, width, 0).astype(jnp.float32).reshape(width, KV_HEADS, HD)
        val_block = lax.dynamic_slice_in_dim(vals_pad, begin, width, 0).astype(jnp.float32).reshape(width, KV_HEADS, HD)
        query_pos = begin + jnp.arange(TOK_DEV, dtype=jnp.int32)
        key_pos = begin - lead + jnp.arange(width, dtype=jnp.int32)
        query_req = lax.dynamic_slice_in_dim(requests.astype(jnp.int32), begin, TOK_DEV, 0)
        key_req = lax.dynamic_slice_in_dim(req_pad, begin, width, 0)
        allowed = (query_req[:, None] == key_req[None, :]) & (key_pos[None, :] <= query_pos[:, None]) & (key_pos[None, :] >= 0)
        wide = allowed[:, None, None, None, :]
        scores = jnp.einsum('tlcqd,kcd->tlcqk', query_block, key_block) * scale
        masked = jnp.where(wide, scores, jnp.float32(-1e+30))
        top = lax.optimization_barrier(jnp.max(masked, axis=-1))
        weights = jnp.where(wide, jnp.exp(masked - top[..., None]), jnp.float32(0.0))
        totals = lax.optimization_barrier(jnp.sum(weights, axis=-1))
        rounded = lax.optimization_barrier(weights.astype(jnp.bfloat16))
        summed = jnp.einsum('tlcqk,kcd->tlcqd', rounded.astype(jnp.float32), val_block)
        result = (summed / totals[..., None]).astype(jnp.bfloat16)
        return result.reshape(TOK_DEV, LAYERS, KV_HEADS * QPER * HD)
    attended = lax.map(one_block, jnp.arange(TOKENS // TOK_DEV, dtype=jnp.int32))
    attended = attended.reshape(TOKENS, LAYERS, KV_HEADS * QPER * HD)
    key_pages = keys.reshape(PAGES, PAGE, KV_HEADS, HD)
    val_pages = values.reshape(PAGES, PAGE, KV_HEADS, HD)
    blocks = jnp.concatenate([key_pages, val_pages], axis=3).transpose(0, 2, 1, 3)
    blocks = blocks.reshape(PAGES * KV_HEADS, PAGE, 2 * HD)
    heads = jnp.arange(KV_HEADS, dtype=jnp.int32)
    target = (page_owner * N_HEAD + heads[None, :] // KV_LOCAL) * SLOTS + page_slot
    cache_pages = jnp.zeros((N_SEQ * N_HEAD * SLOTS, PAGE, 2 * HD), blocks.dtype)
    cache_pages = cache_pages.at[target.reshape(-1).astype(jnp.int32)].set(blocks)
    return (attended, cache_pages)
```

```python
import functools
import math

import jax
import jax.numpy as jnp
from jax import lax
from jax.experimental import pallas as pl
from jax.experimental.pallas import tpu as pltpu
from jax.sharding import PartitionSpec as P

LAYERS = 3
QPER = 5
HD = 128
PAGE = 4
REACH = 8
MESH = pl.DeviceIdType.MESH

masked_score = -16384.0
exponent_scale = math.log2(math.e) / math.sqrt(HD)


def ring_attention(
    seq_count, q_ref, k_ref, v_ref, len_ref, o_ref,
    qs, kbuf, vbuf, bias, eye, ones, top, acc, total, send_sem, recv_sem,
):
    rows = k_ref.shape[0]
    kv_local = kbuf.shape[0]
    mine = lax.axis_index("seq")
    right = lax.rem(mine + 1, seq_count)
    left = lax.rem(mine + seq_count - 1, seq_count)

    barrier = pltpu.get_barrier_semaphore()
    pl.semaphore_signal(barrier, inc=1, device_id={"seq": left}, device_id_type=MESH)
    pl.semaphore_wait(barrier, 1)

    def hop(part, c, slot):
        held = (kbuf, vbuf)[part]
        if isinstance(slot, int) and slot == 1:
            src = (k_ref, v_ref)[part].at[:, pl.ds(c * HD, HD)]
        else:
            src = held.at[c, pl.ds(pl.multiple_of((slot - 1) * rows, rows), rows)]
        return pltpu.make_async_remote_copy(
            src_ref=src,
            dst_ref=held.at[c, pl.ds(pl.multiple_of(slot * rows, rows), rows)],
            send_sem=send_sem.at[slot - 1, c, part],
            recv_sem=recv_sem.at[slot - 1, c, part],
            device_id={"seq": right},
            device_id_type=MESH,
        )

    pieces = [(part, c) for c in range(kv_local) for part in range(2)]
    for part, c in pieces:
        hop(part, c, 1).start()

    for c in range(kv_local):
        kbuf[c, pl.ds(0, rows)] = k_ref[:, c * HD:(c + 1) * HD]
        vbuf[c, pl.ds(0, rows)] = v_ref[:, c * HD:(c + 1) * HD]
        for layer in range(LAYERS):
            for i in range(QPER):
                h = c * QPER + i
                qs[c, layer, pl.ds(i * rows, rows)] = q_ref[layer, :, h * HD:(h + 1) * HD]
    reqs = len_ref.shape[1]
    lengths = len_ref[...].astype(jnp.float32)
    before = lax.broadcasted_iota(jnp.int32, (reqs, reqs), 1) < lax.broadcasted_iota(
        jnp.int32, (reqs, reqs), 0
    )
    starts = jnp.sum(
        jnp.where(before, jnp.broadcast_to(lengths, (reqs, reqs)), 0.0), axis=1, keepdims=True
    )
    query_pos = (mine * rows + lax.broadcasted_iota(jnp.int32, (reqs, rows), 1)).astype(jnp.float32)
    began = jnp.max(jnp.where(starts <= query_pos, starts, 0.0), axis=0, keepdims=True)
    token = (mine * rows + lax.broadcasted_iota(jnp.int32, (rows, rows), 1)).astype(jnp.float32)
    row_iota = lax.broadcasted_iota(jnp.int32, (rows, rows), 0)
    for d in range(REACH + 1):
        key_pos = ((mine - d) * rows + row_iota).astype(jnp.float32)
        allowed = (key_pos >= began) & (key_pos <= token)
        bias[pl.ds(d * rows, rows)] = jnp.where(allowed, 0.0, masked_score).astype(jnp.bfloat16)
    same = (row_iota == lax.broadcasted_iota(jnp.int32, (rows, rows), 1)).astype(jnp.bfloat16)
    for i in range(QPER):
        eye[pl.ds(i * rows, rows)] = same.astype(jnp.bfloat16)
    ones[...] = jnp.ones_like(ones)
    top[...] = jnp.full_like(top, -1e30)
    acc[...] = jnp.zeros_like(acc)
    total[...] = jnp.zeros_like(total)

    def piece(c, layer, first, count):
        span = pl.ds(first, count)
        wide_q = jnp.concatenate([qs[c, layer], eye[...]], axis=1)
        wide_k = jnp.concatenate([kbuf[c, span], bias[span]], axis=1)
        scores = lax.dot_general(
            wide_q, wide_k, (((1,), (1,)), ((), ())), preferred_element_type=jnp.float32
        )
        old = top[c, layer]
        fresh = jnp.maximum(old, jnp.max(scores, axis=1, keepdims=True))
        weights = jnp.exp2((scores - fresh[:, :1]) * exponent_scale)
        shrink = jnp.exp2((old - fresh) * exponent_scale)
        wide_v = jnp.concatenate([vbuf[c, span], ones[pl.ds(0, count)]], axis=1)
        product = jnp.dot(weights.astype(jnp.bfloat16), wide_v, preferred_element_type=jnp.float32)
        top[c, layer] = fresh
        acc[c, layer] = acc[c, layer] * shrink + product[:, :HD]
        total[c, layer] = total[c, layer] * shrink + product[:, HD:]

    def receive(slot, forward):
        for part, c in pieces:
            hop(part, c, slot).wait_recv()
            if forward:
                hop(part, c, slot + 1).start()

    receive(1, True)

    def step(j, carry):
        receive(j + 2, True)
        c = lax.rem(j, kv_local)
        first = pl.multiple_of((j // kv_local) * 2 * rows, 2 * rows)

        def one_layer(layer, carry):
            piece(c, layer, first, 2 * rows)
            return carry

        return lax.fori_loop(0, LAYERS, one_layer, carry)

    lax.fori_loop(0, REACH - 2, step, 0)
    receive(REACH, False)
    near = (REACH - 2) * rows

    def last(layer, carry):
        for c in range(kv_local):
            piece(c, layer, near, 3 * rows)
            done = acc[c, layer] / total[c, layer]
            for i in range(QPER):
                h = c * QPER + i
                o_ref[layer, :, h * HD:(h + 1) * HD] = done[i * rows:(i + 1) * rows].astype(o_ref.dtype)
        return carry

    lax.fori_loop(0, LAYERS, last, 0)
    for slot in range(1, REACH + 1):
        for part, c in pieces:
            hop(part, c, slot).wait_send()


def attend(queries, keys, values, lengths):
    rows = keys.shape[0]
    kv_local = keys.shape[1] // HD
    seq_count = lax.axis_size("seq")
    width = queries.shape[2]
    wide = QPER * rows
    out = pl.pallas_call(
        functools.partial(ring_attention, seq_count),
        name="ring_attention",
        out_shape=jax.ShapeDtypeStruct((LAYERS, rows, width), jnp.bfloat16),
        in_specs=[pl.BlockSpec(memory_space=pltpu.VMEM)] * 4,
        out_specs=pl.BlockSpec(memory_space=pltpu.VMEM),
        scratch_shapes=[
            pltpu.VMEM((kv_local, LAYERS, wide, HD), jnp.bfloat16),
            pltpu.VMEM((kv_local, (REACH + 1) * rows, HD), jnp.bfloat16),
            pltpu.VMEM((kv_local, (REACH + 1) * rows, HD), jnp.bfloat16),
            pltpu.VMEM(((REACH + 1) * rows, rows), jnp.bfloat16),
            pltpu.VMEM((wide, rows), jnp.bfloat16),
            pltpu.VMEM((3 * rows, HD), jnp.bfloat16),
            pltpu.VMEM((kv_local, LAYERS, wide, HD), jnp.float32),
            pltpu.VMEM((kv_local, LAYERS, wide, HD), jnp.float32),
            pltpu.VMEM((kv_local, LAYERS, wide, HD), jnp.float32),
            pltpu.SemaphoreType.DMA((REACH, kv_local, 2)),
            pltpu.SemaphoreType.DMA((REACH, kv_local, 2)),
        ],
        compiler_params=pltpu.CompilerParams(
            collective_id=0, has_side_effects=True, vmem_limit_bytes=56 * 1024 * 1024
        ),
    )(queries.transpose(1, 0, 2), keys, values, lengths.reshape(1, -1))
    return out.transpose(1, 0, 2)


def shards(queries, keys, values, lengths, page_owner, page_slot):
    tok_rows = keys.shape[0]
    kv_local = keys.shape[1] // HD
    seq_count = lax.axis_size("seq")
    pages_dev = tok_rows // PAGE
    slots = pages_dev * kv_local
    key_pages = keys.reshape(pages_dev, PAGE, kv_local, HD)
    val_pages = values.reshape(pages_dev, PAGE, kv_local, HD)
    flat_pages = (
        jnp.concatenate([key_pages, val_pages], axis=3)
        .transpose(0, 2, 1, 3)
        .reshape(slots, PAGE * 2 * HD)
    )
    owner = page_owner.reshape(slots)
    slot = page_slot.reshape(slots)
    number = jnp.arange(slots, dtype=jnp.int32)
    tag_lane = jnp.broadcast_to((slot + 1).astype(jnp.bfloat16)[:, None], (slots, HD))
    flat_pages = jnp.concatenate([flat_pages, tag_lane], axis=1)
    lanes = jnp.arange(seq_count, dtype=jnp.int32)
    picker = (lanes[:, None] == owner[None, :]).astype(jnp.bfloat16)
    outgoing = jnp.dot(picker, flat_pages, preferred_element_type=jnp.float32).astype(jnp.bfloat16)
    received = lax.all_to_all(
        outgoing.reshape(seq_count, 1, PAGE * 2 * HD + HD), "seq", split_axis=0, concat_axis=0, tiled=True
    ).reshape(seq_count, PAGE * 2 * HD + HD)
    got_tags = received[:, PAGE * 2 * HD].astype(jnp.int32)
    placer = (got_tags[None, :] == (number + 1)[:, None]).astype(jnp.bfloat16)
    cache_pages = jnp.dot(
        placer, received[:, :PAGE * 2 * HD], preferred_element_type=jnp.float32
    ).astype(jnp.bfloat16)
    cache_pages = cache_pages.reshape(slots, PAGE, 2 * HD)
    attended = attend(queries, keys, values, lengths)
    return (attended, cache_pages)


def solution(mesh):
    placed = (
        P(("group", "seq"), None, "head"),
        P(("group", "seq"), "head"),
        P(("group", "seq"), "head"),
        P("group"),
        P(("group", "seq"), "head"),
        P(("group", "seq"), "head"),
    )
    return jax.shard_map(
        shards,
        mesh=mesh,
        in_specs=placed,
        out_specs=(P(("group", "seq"), None, "head"), P(("group", "seq", "head"), None, None)),
        check_vma=False,
    )
```

```python
import functools
import math

import jax
import jax.numpy as jnp
from jax import lax
from jax.experimental import pallas as pl
from jax.experimental.pallas import tpu as pltpu
from jax.sharding import PartitionSpec as P

LAYERS = 3
QPER = 5
HD = 128
PAGE = 4
REACH = 8
GROUP = 3
MESH = pl.DeviceIdType.MESH

masked_score = -16384.0
exponent_scale = math.log2(math.e) / math.sqrt(HD)


def ring_attention(
    seq_count, q_ref, k_ref, v_ref, len_ref, o_ref,
    qs, held, bias, eye, ones, top, acc, total, send_sem, recv_sem,
):
    rows = k_ref.shape[0]
    kv_local = held.shape[1]
    parts = 2 * kv_local
    mine = lax.axis_index("seq")
    right = lax.rem(mine + 1, seq_count)
    left = lax.rem(mine + seq_count - 1, seq_count)

    barrier = pltpu.get_barrier_semaphore()
    pl.semaphore_signal(barrier, inc=1, device_id={"seq": left}, device_id_type=MESH)
    pl.semaphore_wait(barrier, 1)

    def hop(n, src=None):
        slot = n // parts
        c, part = (n % parts) // 2, n % 2
        if src is None:
            src = held.at[part, c, pl.ds(pl.multiple_of(slot * rows, rows), rows)]
        return pltpu.make_async_remote_copy(
            src_ref=src,
            dst_ref=held.at[part, c, pl.ds(pl.multiple_of((slot + 1) * rows, rows), rows)],
            send_sem=send_sem.at[n],
            recv_sem=recv_sem.at[n],
            device_id={"seq": right},
            device_id_type=MESH,
        )

    for n in range(parts):
        hop(n, (k_ref, v_ref)[n % 2].at[:, pl.ds((n // 2) * HD, HD)]).start()

    for c in range(kv_local):
        held[0, c, pl.ds(0, rows)] = k_ref[:, c * HD:(c + 1) * HD]
        held[1, c, pl.ds(0, rows)] = v_ref[:, c * HD:(c + 1) * HD]
        for layer in range(LAYERS):
            for i in range(QPER):
                h = c * QPER + i
                qs[c, layer, pl.ds(i * rows, rows)] = q_ref[layer, :, h * HD:(h + 1) * HD]
    reqs = len_ref.shape[1]
    lengths = len_ref[...].astype(jnp.float32)
    before = lax.broadcasted_iota(jnp.int32, (reqs, reqs), 1) < lax.broadcasted_iota(
        jnp.int32, (reqs, reqs), 0
    )
    starts = jnp.sum(
        jnp.where(before, jnp.broadcast_to(lengths, (reqs, reqs)), 0.0), axis=1, keepdims=True
    )
    query_pos = (mine * rows + lax.broadcasted_iota(jnp.int32, (reqs, rows), 1)).astype(jnp.float32)
    began = jnp.max(jnp.where(starts <= query_pos, starts, 0.0), axis=0, keepdims=True)
    token = (mine * rows + lax.broadcasted_iota(jnp.int32, (rows, rows), 1)).astype(jnp.float32)
    row_iota = lax.broadcasted_iota(jnp.int32, (rows, rows), 0)
    for d in range(REACH + 1):
        key_pos = ((mine - d) * rows + row_iota).astype(jnp.float32)
        allowed = (key_pos >= began) & (key_pos <= token)
        bias[pl.ds(d * rows, rows)] = jnp.where(allowed, 0.0, masked_score).astype(jnp.bfloat16)
    same = (row_iota == lax.broadcasted_iota(jnp.int32, (rows, rows), 1)).astype(jnp.bfloat16)
    for i in range(QPER):
        eye[pl.ds(i * rows, rows)] = same.astype(jnp.bfloat16)
    ones[...] = jnp.ones_like(ones)
    span = GROUP * rows

    def piece(i, first, last=False):
        c, layer = i // LAYERS, i % LAYERS
        keys = pl.ds(first * rows, span)
        wide_q = jnp.concatenate([qs[c, layer], eye[...]], axis=1)
        wide_k = jnp.concatenate([held[0, c, keys], bias[keys]], axis=1)
        scores = lax.dot_general(
            wide_q, wide_k, (((1,), (1,)), ((), ())), preferred_element_type=jnp.float32
        )
        fresh = jnp.max(scores, axis=1, keepdims=True)
        if first > 0:
            old = top[c, layer]
            fresh = jnp.maximum(old, fresh)
            shrink = jnp.exp2((old - fresh) * exponent_scale)
            fresh = fresh[:, :1]
        weights = jnp.exp2((scores - fresh) * exponent_scale)
        wide_v = jnp.concatenate([held[1, c, keys], ones[...]], axis=1)
        product = jnp.dot(weights.astype(jnp.bfloat16), wide_v, preferred_element_type=jnp.float32)
        summed, counted = product[:, :HD], product[:, HD:]
        if first > 0:
            summed = acc[c, layer] * shrink + summed
            counted = total[c, layer] * shrink + counted
        if last:
            done = (summed / counted).astype(o_ref.dtype)
            for q in range(QPER):
                h = c * QPER + q
                place = h * HD if isinstance(h, int) else pl.multiple_of(h * HD, HD)
                o_ref[layer, :, pl.ds(place, HD)] = done[q * rows:(q + 1) * rows]
        else:
            top[c, layer] = jnp.broadcast_to(fresh, (QPER * rows, HD))
            acc[c, layer] = summed
            total[c, layer] = counted

    def handle(n, forward=True):
        hop(n).wait_recv()
        if forward:
            hop(n + parts).start()

    def loop(count, body):
        def step(i, carry):
            body(i)
            return carry

        lax.fori_loop(0, count, step, 0)

    loop(8, handle)

    def first_group(i):
        handle(8 + 2 * i)
        piece(i, 0)
        handle(9 + 2 * i)

    loop(kv_local * LAYERS, first_group)

    def second_group(i):
        handle(20 + i)
        piece(i, GROUP)

    loop(kv_local * LAYERS, second_group)
    handle(26)
    handle(27)
    handle(28, False)
    handle(29, False)

    def third_group(i):
        @pl.when(i < 2)
        def _():
            handle(30 + i, False)

        piece(i, 2 * GROUP, True)

    loop(kv_local * LAYERS, third_group)
    loop(REACH * parts, lambda n: hop(n).wait_send())


def attend(queries, keys, values, lengths):
    rows = keys.shape[0]
    kv_local = keys.shape[1] // HD
    seq_count = lax.axis_size("seq")
    width = queries.shape[2]
    wide = QPER * rows
    out = pl.pallas_call(
        functools.partial(ring_attention, seq_count),
        name="ring_attention",
        out_shape=jax.ShapeDtypeStruct((LAYERS, rows, width), jnp.bfloat16),
        in_specs=[pl.BlockSpec(memory_space=pltpu.VMEM)] * 4,
        out_specs=pl.BlockSpec(memory_space=pltpu.VMEM),
        scratch_shapes=[
            pltpu.VMEM((kv_local, LAYERS, wide, HD), jnp.bfloat16),
            pltpu.VMEM((2, kv_local, (REACH + 1) * rows, HD), jnp.bfloat16),
            pltpu.VMEM(((REACH + 1) * rows, rows), jnp.bfloat16),
            pltpu.VMEM((wide, rows), jnp.bfloat16),
            pltpu.VMEM((GROUP * rows, HD), jnp.bfloat16),
            pltpu.VMEM((kv_local, LAYERS, wide, HD), jnp.float32),
            pltpu.VMEM((kv_local, LAYERS, wide, HD), jnp.float32),
            pltpu.VMEM((kv_local, LAYERS, wide, HD), jnp.float32),
            pltpu.SemaphoreType.DMA((REACH * kv_local * 2,)),
            pltpu.SemaphoreType.DMA((REACH * kv_local * 2,)),
        ],
        compiler_params=pltpu.CompilerParams(
            collective_id=0, has_side_effects=True, vmem_limit_bytes=56 * 1024 * 1024
        ),
    )(queries.transpose(1, 0, 2), keys, values, lengths.reshape(1, -1))
    return out.transpose(1, 0, 2)


def shards(queries, keys, values, lengths, page_owner, page_slot):
    tok_rows = keys.shape[0]
    kv_local = keys.shape[1] // HD
    seq_count = lax.axis_size("seq")
    pages_dev = tok_rows // PAGE
    slots = pages_dev * kv_local
    key_pages = keys.reshape(pages_dev, PAGE, kv_local, HD)
    val_pages = values.reshape(pages_dev, PAGE, kv_local, HD)
    flat_pages = (
        jnp.concatenate([key_pages, val_pages], axis=3)
        .transpose(0, 2, 1, 3)
        .reshape(slots, PAGE * 2 * HD)
    )
    owner = page_owner.reshape(slots)
    slot = page_slot.reshape(slots)
    number = jnp.arange(slots, dtype=jnp.int32)
    tag_lane = jnp.broadcast_to((slot + 1).astype(jnp.bfloat16)[:, None], (slots, HD))
    flat_pages = jnp.concatenate([flat_pages, tag_lane], axis=1)
    lanes = jnp.arange(seq_count, dtype=jnp.int32)
    picker = (lanes[:, None] == owner[None, :]).astype(jnp.bfloat16)
    outgoing = jnp.dot(picker, flat_pages, preferred_element_type=jnp.float32).astype(jnp.bfloat16)
    received = lax.all_to_all(
        outgoing.reshape(seq_count, 1, PAGE * 2 * HD + HD), "seq", split_axis=0, concat_axis=0, tiled=True
    ).reshape(seq_count, PAGE * 2 * HD + HD)
    got_tags = received[:, PAGE * 2 * HD].astype(jnp.int32)
    placer = (got_tags[None, :] == (number + 1)[:, None]).astype(jnp.bfloat16)
    cache_pages = jnp.dot(
        placer, received[:, :PAGE * 2 * HD], preferred_element_type=jnp.float32
    ).astype(jnp.bfloat16)
    cache_pages = cache_pages.reshape(slots, PAGE, 2 * HD)
    attended = attend(queries, keys, values, lengths)
    return (attended, cache_pages)


def solution(mesh):
    placed = (
        P(("group", "seq"), None, "head"),
        P(("group", "seq"), "head"),
        P(("group", "seq"), "head"),
        P("group"),
        P(("group", "seq"), "head"),
        P(("group", "seq"), "head"),
    )
    return jax.shard_map(
        shards,
        mesh=mesh,
        in_specs=placed,
        out_specs=(P(("group", "seq"), None, "head"), P(("group", "seq", "head"), None, None)),
        check_vma=False,
    )
```

```python
import functools
import math

import jax
import jax.numpy as jnp
from jax import lax
from jax.experimental import pallas as pl
from jax.experimental.pallas import tpu as pltpu
from jax.sharding import PartitionSpec as P

LAYERS = 3
QPER = 5
HD = 128
PAGE = 4
REACH = 8
GROUP = 3
COLUMNS = 4
FIRST_HOPS = 6
MESH = pl.DeviceIdType.MESH

masked_score = -16384.0
exponent_scale = math.log2(math.e) / math.sqrt(HD)


def ring_attention(
    seq_count, q_ref, k_ref, v_ref, len_ref, owner_ref, slot_ref, o_ref, page_ref,
    qs, held, bias, eye, ones, top, acc, total, send_sem, recv_sem,
    picked, across, along, landed, tag_across, tag_along, tag_landed,
    across_send, across_recv, along_send, along_recv, from_right, from_left,
):
    rows = k_ref.shape[0]
    kv_local = held.shape[1]
    parts = 2 * kv_local
    mine = lax.axis_index("seq")
    right = lax.rem(mine + 1, seq_count)
    left = lax.rem(mine + seq_count - 1, seq_count)

    places = seq_count // COLUMNS
    column, place = mine // places, lax.rem(mine, places)

    def at_place(offset):
        return column * places + lax.rem(place + places + offset, places)

    def at_column(offset):
        return lax.rem(column + COLUMNS + offset, COLUMNS) * places + place

    def signal(sem, device):
        pl.semaphore_signal(sem, inc=1, device_id={"seq": device}, device_id_type=MESH)

    barrier = pltpu.get_barrier_semaphore()
    signal(barrier, left)
    signal(barrier, at_place(1))
    signal(barrier, at_place(-1))
    for offset in range(1, COLUMNS):
        signal(barrier, at_column(offset))
    pl.semaphore_wait(barrier, COLUMNS + 2)
    signal(from_right, at_place(-1))
    signal(from_left, at_place(1))

    def hop(n, src=None):
        slot = n // parts
        c, part = (n % parts) // 2, n % 2
        if src is None:
            src = held.at[part, c, pl.ds(pl.multiple_of(slot * rows, rows), rows)]
        return pltpu.make_async_remote_copy(
            src_ref=src,
            dst_ref=held.at[part, c, pl.ds(pl.multiple_of((slot + 1) * rows, rows), rows)],
            send_sem=send_sem.at[n],
            recv_sem=recv_sem.at[n],
            device_id={"seq": right},
            device_id_type=MESH,
        )

    for n in range(parts):
        hop(n, (k_ref, v_ref)[n % 2].at[:, pl.ds((n // 2) * HD, HD)]).start()

    lines = places * PAGE
    unit = COLUMNS * PAGE

    def iota(shape, axis):
        return lax.broadcasted_iota(jnp.int32, shape, axis)

    pages_dev = rows // PAGE
    widen = (iota((pages_dev, rows), 0) == iota((pages_dev, rows), 1) // PAGE).astype(jnp.bfloat16)

    def per_token(ref):
        wide = jnp.dot(
            ref[...].astype(jnp.float32).astype(jnp.bfloat16), widen, preferred_element_type=jnp.float32
        )
        return jnp.concatenate([wide[c:c + 1] for c in range(kv_local)], axis=1)

    owner_row = per_token(owner_ref)
    slot_row = per_token(slot_ref) + 1.0
    line_row = (iota((1, kv_local * rows), 1) % PAGE).astype(jnp.float32)
    goes = iota((seq_count * PAGE, kv_local * rows), 0).astype(jnp.float32) == owner_row * PAGE + line_row
    source = jnp.concatenate(
        [
            jnp.concatenate(
                [k_ref[:, c * HD:(c + 1) * HD], v_ref[:, c * HD:(c + 1) * HD]], axis=1
            )
            for c in range(kv_local)
        ],
        axis=0,
    )

    def one_hot(mask):
        return jnp.where(mask, 1.0, 0.0).astype(jnp.bfloat16)

    picked[...] = jnp.dot(one_hot(goes), source, preferred_element_type=jnp.float32).astype(jnp.bfloat16)
    owned = (iota((seq_count, kv_local * rows), 0).astype(jnp.float32) == owner_row) & (
        jnp.broadcast_to(line_row, (seq_count, kv_local * rows)) == 0.0
    )
    tags = lax.dot_general(
        jnp.broadcast_to(slot_row, (8, kv_local * rows)).astype(jnp.bfloat16),
        one_hot(owned),
        (((1,), (1,)), ((), ())),
        preferred_element_type=jnp.float32,
    )
    tag_across[column] = tags[:1]
    own_lines = pl.ds(pl.multiple_of(column * lines, lines), lines)
    across[own_lines] = picked[own_lines]

    def to_column(offset):
        device = at_column(offset)
        first = pl.multiple_of((device // places) * lines, lines)
        return [
            pltpu.make_async_remote_copy(
                src_ref=src,
                dst_ref=dst,
                send_sem=across_send.at[part, offset],
                recv_sem=across_recv.at[part, offset],
                device_id={"seq": device},
                device_id_type=MESH,
            )
            for part, (src, dst) in enumerate(
                (
                    (picked.at[pl.ds(first, lines)], across.at[own_lines]),
                    (tag_across.at[column], tag_across.at[column]),
                )
            )
        ]

    def to_place(offset, landing):
        device = at_place(offset)
        there = lax.rem(device, places)
        return [
            pltpu.make_async_remote_copy(
                src_ref=src,
                dst_ref=dst,
                send_sem=along_send.at[part, landing],
                recv_sem=along_recv.at[part, landing],
                device_id={"seq": device},
                device_id_type=MESH,
            )
            for part, (src, dst) in enumerate(
                (
                    (
                        along.at[pl.ds(pl.multiple_of(there * unit, unit), unit)],
                        landed.at[pl.ds(pl.multiple_of(landing * unit, unit), unit)],
                    ),
                    (tag_along.at[there], tag_landed.at[landing]),
                )
            )
        ]

    for c in range(kv_local):
        held[0, c, pl.ds(0, rows)] = k_ref[:, c * HD:(c + 1) * HD]
        held[1, c, pl.ds(0, rows)] = v_ref[:, c * HD:(c + 1) * HD]
        for layer in range(LAYERS):
            for i in range(QPER):
                h = c * QPER + i
                qs[c, layer, pl.ds(i * rows, rows)] = q_ref[layer, :, h * HD:(h + 1) * HD]
    reqs = len_ref.shape[1]
    lengths = len_ref[...].astype(jnp.float32)
    before = lax.broadcasted_iota(jnp.int32, (reqs, reqs), 1) < lax.broadcasted_iota(
        jnp.int32, (reqs, reqs), 0
    )
    starts = jnp.sum(
        jnp.where(before, jnp.broadcast_to(lengths, (reqs, reqs)), 0.0), axis=1, keepdims=True
    )
    query_pos = (mine * rows + lax.broadcasted_iota(jnp.int32, (reqs, rows), 1)).astype(jnp.float32)
    began = jnp.max(jnp.where(starts <= query_pos, starts, 0.0), axis=0, keepdims=True)
    token = (mine * rows + lax.broadcasted_iota(jnp.int32, (rows, rows), 1)).astype(jnp.float32)
    row_iota = lax.broadcasted_iota(jnp.int32, (rows, rows), 0)
    for d in range(REACH + 1):
        key_pos = ((mine - d) * rows + row_iota).astype(jnp.float32)
        allowed = (key_pos >= began) & (key_pos <= token)
        bias[pl.ds(d * rows, rows)] = jnp.where(allowed, 0.0, masked_score).astype(jnp.bfloat16)
    same = (row_iota == lax.broadcasted_iota(jnp.int32, (rows, rows), 1)).astype(jnp.bfloat16)
    for i in range(QPER):
        eye[pl.ds(i * rows, rows)] = same.astype(jnp.bfloat16)
    ones[...] = jnp.ones_like(ones)
    span = GROUP * rows

    def piece(i, first, last=False):
        c, layer = i // LAYERS, i % LAYERS
        keys = pl.ds(first * rows, span)
        wide_q = jnp.concatenate([qs[c, layer], eye[...]], axis=1)
        wide_k = jnp.concatenate([held[0, c, keys], bias[keys]], axis=1)
        scores = lax.dot_general(
            wide_q, wide_k, (((1,), (1,)), ((), ())), preferred_element_type=jnp.float32
        )
        fresh = jnp.max(scores, axis=1, keepdims=True)
        if first > 0:
            old = top[c, layer]
            fresh = jnp.maximum(old, fresh)
            shrink = jnp.exp2((old - fresh) * exponent_scale)
            fresh = fresh[:, :1]
        weights = jnp.exp2((scores - fresh) * exponent_scale)
        wide_v = jnp.concatenate([held[1, c, keys], ones[...]], axis=1)
        product = jnp.dot(weights.astype(jnp.bfloat16), wide_v, preferred_element_type=jnp.float32)
        summed, counted = product[:, :HD], product[:, HD:]
        if first > 0:
            summed = acc[c, layer] * shrink + summed
            counted = total[c, layer] * shrink + counted
        if last:
            done = (summed / counted).astype(o_ref.dtype)
            for q in range(QPER):
                h = c * QPER + q
                place = h * HD if isinstance(h, int) else pl.multiple_of(h * HD, HD)
                o_ref[layer, :, pl.ds(place, HD)] = done[q * rows:(q + 1) * rows]
        else:
            top[c, layer] = jnp.broadcast_to(fresh, (QPER * rows, HD))
            acc[c, layer] = summed
            total[c, layer] = counted

    def handle(n, forward=True):
        hop(n).wait_recv()
        if forward:
            hop(n + parts).start()

    def loop(count, body):
        def step(i, carry):
            body(i)
            return carry

        lax.fori_loop(0, count, step, 0)

    for offset in range(1, COLUMNS):
        for copy in to_column(offset):
            copy.start()

    half = places // 2

    def next_token(more):
        pl.semaphore_wait(from_right, 1)
        pl.semaphore_wait(from_left, 1)

        @pl.when(more)
        def _():
            signal(from_right, at_place(-1))
            signal(from_left, at_place(1))

    def send_both(k):
        for copy in to_place(k, k):
            copy.start()

        @pl.when(k < half)
        def _():
            for copy in to_place(-k, half + k):
                copy.start()

    def early(i):
        next_token(i >= 0)
        handle(i)

    loop(FIRST_HOPS - 1, early)
    for offset in range(1, COLUMNS):
        for copy in to_column(offset):
            copy.wait_recv()
    row = iota((seq_count * PAGE, seq_count * PAGE), 0)
    regroup = (row % unit) // PAGE * lines + row // unit * PAGE + row % PAGE
    along[...] = jnp.dot(
        one_hot(regroup == iota((seq_count * PAGE, seq_count * PAGE), 1)),
        across[...],
        preferred_element_type=jnp.float32,
    ).astype(jnp.bfloat16)
    tag_rows = jnp.zeros((HD, seq_count), jnp.float32)
    for x in range(COLUMNS):
        mask = (iota((HD, seq_count), 0) % unit) // PAGE == x
        tag_rows = jnp.where(mask, jnp.broadcast_to(tag_across[x], (HD, seq_count)), tag_rows)
    choose = iota((places, seq_count), 1) == column * places + iota((places, seq_count), 0)
    tag_table = lax.dot_general(
        one_hot(choose),
        tag_rows.astype(jnp.bfloat16),
        (((1,), (1,)), ((), ())),
        preferred_element_type=jnp.float32,
    )
    for z in range(places):
        tag_along[z] = tag_table[z:z + 1]
    landed[pl.ds(0, unit)] = along[pl.ds(pl.multiple_of(place * unit, unit), unit)]
    tag_landed[0] = tag_along[place]
    loop(FIRST_HOPS, lambda i: send_both(i + 1))

    def late(i):
        k = i + FIRST_HOPS + 1
        next_token(k < half)
        handle(k - 2)
        send_both(k)

    loop(half - FIRST_HOPS, late)
    done_chunks = half - 1
    pieces = kv_local * LAYERS

    def first_group(i):
        handle(done_chunks + i)
        piece(i, 0)

    loop(pieces, first_group)

    def second_group(i):
        handle(done_chunks + pieces + i)
        piece(i, GROUP)

    loop(pieces, second_group)
    last_chunks = (REACH - 1) * parts
    for n in range(done_chunks + 2 * pieces, last_chunks + 2):
        handle(n, n < last_chunks)

    def wait_pages(i):
        for copy in to_place(1, i + 1):
            copy.wait_recv()

    loop(places - 1, wait_pages)
    came = jnp.concatenate([tag_landed[z] for z in range(places)], axis=0)
    spread = jnp.dot(
        one_hot(iota((seq_count * PAGE, places), 0) // unit == iota((seq_count * PAGE, places), 1)),
        came.astype(jnp.bfloat16),
        preferred_element_type=jnp.float32,
    )
    here = iota((seq_count * PAGE, HD), 0) % unit == iota((seq_count * PAGE, HD), 1)
    tag_column = jnp.sum(jnp.where(here, spread, 0.0), axis=1, keepdims=True)
    line_column = (iota((seq_count * PAGE, 1), 0) % PAGE).astype(jnp.float32)
    lands = (tag_column - 1.0) * PAGE + line_column
    slot_lines = page_ref.shape[0]
    put = iota((seq_count * PAGE, slot_lines), 1).astype(jnp.float32) == lands
    page_ref[...] = lax.dot_general(
        one_hot(put), landed[...], (((0,), (0,)), ((), ())), preferred_element_type=jnp.float32
    ).astype(page_ref.dtype)

    def third_group(i):
        @pl.when(i < 2)
        def _():
            handle(last_chunks + 2 + i, False)

        piece(i, 2 * GROUP, True)

    loop(pieces, third_group)
    loop(REACH * parts, lambda n: hop(n).wait_send())
    for offset in range(1, COLUMNS):
        for copy in to_column(offset):
            copy.wait_send()

    def wait_sent(i):
        for copy in to_place(1, i + 1):
            copy.wait_send()

    loop(places - 1, wait_sent)


def shards(queries, keys, values, lengths, page_owner, page_slot):
    rows = keys.shape[0]
    kv_local = keys.shape[1] // HD
    seq_count = lax.axis_size("seq")
    width = queries.shape[2]
    wide = QPER * rows
    pages_dev = rows // PAGE
    slots = pages_dev * kv_local
    places = seq_count // COLUMNS
    lines = seq_count * PAGE
    attended, pages = pl.pallas_call(
        functools.partial(ring_attention, seq_count),
        name="ring_attention",
        out_shape=(
            jax.ShapeDtypeStruct((LAYERS, rows, width), jnp.bfloat16),
            jax.ShapeDtypeStruct((slots * PAGE, 2 * HD), jnp.bfloat16),
        ),
        in_specs=[pl.BlockSpec(memory_space=pltpu.VMEM)] * 6,
        out_specs=(pl.BlockSpec(memory_space=pltpu.VMEM), pl.BlockSpec(memory_space=pltpu.VMEM)),
        scratch_shapes=[
            pltpu.VMEM((kv_local, LAYERS, wide, HD), jnp.bfloat16),
            pltpu.VMEM((2, kv_local, (REACH + 1) * rows, HD), jnp.bfloat16),
            pltpu.VMEM(((REACH + 1) * rows, rows), jnp.bfloat16),
            pltpu.VMEM((wide, rows), jnp.bfloat16),
            pltpu.VMEM((GROUP * rows, HD), jnp.bfloat16),
            pltpu.VMEM((kv_local, LAYERS, wide, HD), jnp.float32),
            pltpu.VMEM((kv_local, LAYERS, wide, HD), jnp.float32),
            pltpu.VMEM((kv_local, LAYERS, wide, HD), jnp.float32),
            pltpu.SemaphoreType.DMA((REACH * kv_local * 2,)),
            pltpu.SemaphoreType.DMA((REACH * kv_local * 2,)),
            pltpu.VMEM((lines, 2 * HD), jnp.bfloat16),
            pltpu.VMEM((lines, 2 * HD), jnp.bfloat16),
            pltpu.VMEM((lines, 2 * HD), jnp.bfloat16),
            pltpu.VMEM((lines, 2 * HD), jnp.bfloat16),
            pltpu.VMEM((COLUMNS, 1, seq_count), jnp.float32),
            pltpu.VMEM((places, 1, HD), jnp.float32),
            pltpu.VMEM((places, 1, HD), jnp.float32),
            pltpu.SemaphoreType.DMA((2, COLUMNS)),
            pltpu.SemaphoreType.DMA((2, COLUMNS)),
            pltpu.SemaphoreType.DMA((2, places)),
            pltpu.SemaphoreType.DMA((2, places)),
            pltpu.SemaphoreType.REGULAR,
            pltpu.SemaphoreType.REGULAR,
        ],
        compiler_params=pltpu.CompilerParams(
            collective_id=0, has_side_effects=True, vmem_limit_bytes=56 * 1024 * 1024
        ),
    )(
        queries.transpose(1, 0, 2), keys, values, lengths.reshape(1, -1),
        page_owner.transpose(1, 0), page_slot.transpose(1, 0),
    )
    return (attended.transpose(1, 0, 2), pages.reshape(slots, PAGE, 2 * HD))


def solution(mesh):
    placed = (
        P(("group", "seq"), None, "head"),
        P(("group", "seq"), "head"),
        P(("group", "seq"), "head"),
        P("group"),
        P(("group", "seq"), "head"),
        P(("group", "seq"), "head"),
    )
    return jax.shard_map(
        shards,
        mesh=mesh,
        in_specs=placed,
        out_specs=(P(("group", "seq"), None, "head"), P(("group", "seq", "head"), None, None)),
        check_vma=False,
    )
```

```python
import functools
import math

import jax
import jax.numpy as jnp
from jax import lax
from jax.experimental import pallas as pl
from jax.experimental.pallas import tpu as pltpu
from jax.sharding import PartitionSpec as P

LAYERS = 3
QPER = 5
HD = 128
PAGE = 4
REACH = 8
GROUP = 3
COLUMNS = 4
STOP = 8
FORWARD = 12
MESH = pl.DeviceIdType.MESH

masked_score = -16384.0
exponent_scale = math.log2(math.e) / math.sqrt(HD)


def ring_attention(
    seq_count, q_ref, k_ref, v_ref, len_ref, owner_ref, slot_ref, o_ref, page_ref,
    qs, held, bias, eye, ones, top, acc, total, send_sem, recv_sem,
    picked, across, along, landed, tag_across, tag_along, tag_landed,
    stopped, tag_stopped,
    across_send, across_recv, along_send, along_recv, stop_send, stop_recv, from_right, from_left,
):
    rows = k_ref.shape[0]
    kv_local = held.shape[1]
    parts = 2 * kv_local
    mine = lax.axis_index("seq")
    right = lax.rem(mine + 1, seq_count)
    left = lax.rem(mine + seq_count - 1, seq_count)

    places = seq_count // COLUMNS
    column, place = mine // places, lax.rem(mine, places)

    def at_place(offset):
        return column * places + lax.rem(place + places + offset, places)

    def at_column(offset):
        return lax.rem(column + COLUMNS + offset, COLUMNS) * places + place

    def signal(sem, device):
        pl.semaphore_signal(sem, inc=1, device_id={"seq": device}, device_id_type=MESH)

    barrier = pltpu.get_barrier_semaphore()
    signal(barrier, left)
    signal(barrier, at_place(1))
    signal(barrier, at_place(-1))
    for offset in range(1, COLUMNS):
        signal(barrier, at_column(offset))
    pl.semaphore_wait(barrier, COLUMNS + 2)
    signal(from_right, at_place(-1))
    signal(from_left, at_place(1))

    def hop(n, src=None):
        slot = n // parts
        c, part = (n % parts) // 2, n % 2
        if src is None:
            src = held.at[part, c, pl.ds(pl.multiple_of(slot * rows, rows), rows)]
        return pltpu.make_async_remote_copy(
            src_ref=src,
            dst_ref=held.at[part, c, pl.ds(pl.multiple_of((slot + 1) * rows, rows), rows)],
            send_sem=send_sem.at[n],
            recv_sem=recv_sem.at[n],
            device_id={"seq": right},
            device_id_type=MESH,
        )

    for n in range(parts):
        hop(n, (k_ref, v_ref)[n % 2].at[:, pl.ds((n // 2) * HD, HD)]).start()

    lines = places * PAGE
    unit = COLUMNS * PAGE

    def iota(shape, axis):
        return lax.broadcasted_iota(jnp.int32, shape, axis)

    pages_dev = rows // PAGE
    widen = (iota((pages_dev, rows), 0) == iota((pages_dev, rows), 1) // PAGE).astype(jnp.bfloat16)

    def per_token(ref):
        wide = jnp.dot(
            ref[...].astype(jnp.float32).astype(jnp.bfloat16), widen, preferred_element_type=jnp.float32
        )
        return jnp.concatenate([wide[c:c + 1] for c in range(kv_local)], axis=1)

    owner_row = per_token(owner_ref)
    slot_row = per_token(slot_ref) + 1.0
    line_row = (iota((1, kv_local * rows), 1) % PAGE).astype(jnp.float32)
    goes = iota((seq_count * PAGE, kv_local * rows), 0).astype(jnp.float32) == owner_row * PAGE + line_row
    source = jnp.concatenate(
        [
            jnp.concatenate(
                [k_ref[:, c * HD:(c + 1) * HD], v_ref[:, c * HD:(c + 1) * HD]], axis=1
            )
            for c in range(kv_local)
        ],
        axis=0,
    )

    def one_hot(mask):
        return jnp.where(mask, 1.0, 0.0).astype(jnp.bfloat16)

    picked[...] = jnp.dot(one_hot(goes), source, preferred_element_type=jnp.float32).astype(jnp.bfloat16)
    owned = (iota((seq_count, kv_local * rows), 0).astype(jnp.float32) == owner_row) & (
        jnp.broadcast_to(line_row, (seq_count, kv_local * rows)) == 0.0
    )
    tags = lax.dot_general(
        jnp.broadcast_to(slot_row, (8, kv_local * rows)).astype(jnp.bfloat16),
        one_hot(owned),
        (((1,), (1,)), ((), ())),
        preferred_element_type=jnp.float32,
    )
    tag_across[column] = tags[:1]
    own_lines = pl.ds(pl.multiple_of(column * lines, lines), lines)
    across[own_lines] = picked[own_lines]

    def to_column(offset):
        device = at_column(offset)
        first = pl.multiple_of((device // places) * lines, lines)
        return [
            pltpu.make_async_remote_copy(
                src_ref=src,
                dst_ref=dst,
                send_sem=across_send.at[part, offset],
                recv_sem=across_recv.at[part, offset],
                device_id={"seq": device},
                device_id_type=MESH,
            )
            for part, (src, dst) in enumerate(
                (
                    (picked.at[pl.ds(first, lines)], across.at[own_lines]),
                    (tag_across.at[column], tag_across.at[column]),
                )
            )
        ]

    def to_place(offset, landing):
        device = at_place(offset)
        there = lax.rem(device, places)
        return [
            pltpu.make_async_remote_copy(
                src_ref=src,
                dst_ref=dst,
                send_sem=along_send.at[part, landing],
                recv_sem=along_recv.at[part, landing],
                device_id={"seq": device},
                device_id_type=MESH,
            )
            for part, (src, dst) in enumerate(
                (
                    (
                        along.at[pl.ds(pl.multiple_of(there * unit, unit), unit)],
                        landed.at[pl.ds(pl.multiple_of(landing * unit, unit), unit)],
                    ),
                    (tag_along.at[there], tag_landed.at[landing]),
                )
            )
        ]

    for c in range(kv_local):
        held[0, c, pl.ds(0, rows)] = k_ref[:, c * HD:(c + 1) * HD]
        held[1, c, pl.ds(0, rows)] = v_ref[:, c * HD:(c + 1) * HD]
        for layer in range(LAYERS):
            for i in range(QPER):
                h = c * QPER + i
                qs[c, layer, pl.ds(i * rows, rows)] = q_ref[layer, :, h * HD:(h + 1) * HD]
    reqs = len_ref.shape[1]
    lengths = len_ref[...].astype(jnp.float32)
    before = lax.broadcasted_iota(jnp.int32, (reqs, reqs), 1) < lax.broadcasted_iota(
        jnp.int32, (reqs, reqs), 0
    )
    starts = jnp.sum(
        jnp.where(before, jnp.broadcast_to(lengths, (reqs, reqs)), 0.0), axis=1, keepdims=True
    )
    query_pos = (mine * rows + lax.broadcasted_iota(jnp.int32, (reqs, rows), 1)).astype(jnp.float32)
    began = jnp.max(jnp.where(starts <= query_pos, starts, 0.0), axis=0, keepdims=True)
    token = (mine * rows + lax.broadcasted_iota(jnp.int32, (rows, rows), 1)).astype(jnp.float32)
    row_iota = lax.broadcasted_iota(jnp.int32, (rows, rows), 0)
    for d in range(REACH + 1):
        key_pos = ((mine - d) * rows + row_iota).astype(jnp.float32)
        allowed = (key_pos >= began) & (key_pos <= token)
        bias[pl.ds(d * rows, rows)] = jnp.where(allowed, 0.0, masked_score).astype(jnp.bfloat16)
    same = (row_iota == lax.broadcasted_iota(jnp.int32, (rows, rows), 1)).astype(jnp.bfloat16)
    for i in range(QPER):
        eye[pl.ds(i * rows, rows)] = same.astype(jnp.bfloat16)
    ones[...] = jnp.ones_like(ones)
    span = GROUP * rows

    def piece(i, first, last=False):
        c, layer = i // LAYERS, i % LAYERS
        keys = pl.ds(first * rows, span)
        wide_q = jnp.concatenate([qs[c, layer], eye[...]], axis=1)
        wide_k = jnp.concatenate([held[0, c, keys], bias[keys]], axis=1)
        scores = lax.dot_general(
            wide_q, wide_k, (((1,), (1,)), ((), ())), preferred_element_type=jnp.float32
        )
        fresh = jnp.max(scores, axis=1, keepdims=True)
        if first > 0:
            old = top[c, layer]
            fresh = jnp.maximum(old, fresh)
            shrink = jnp.exp2((old - fresh) * exponent_scale)
            fresh = fresh[:, :1]
        weights = jnp.exp2((scores - fresh) * exponent_scale)
        wide_v = jnp.concatenate([held[1, c, keys], ones[...]], axis=1)
        product = jnp.dot(weights.astype(jnp.bfloat16), wide_v, preferred_element_type=jnp.float32)
        summed, counted = product[:, :HD], product[:, HD:]
        if first > 0:
            summed = acc[c, layer] * shrink + summed
            counted = total[c, layer] * shrink + counted
        if last:
            done = (summed / counted).astype(o_ref.dtype)
            for q in range(QPER):
                h = c * QPER + q
                place = h * HD if isinstance(h, int) else pl.multiple_of(h * HD, HD)
                o_ref[layer, :, pl.ds(place, HD)] = done[q * rows:(q + 1) * rows]
        else:
            top[c, layer] = jnp.broadcast_to(fresh, (QPER * rows, HD))
            acc[c, layer] = summed
            total[c, layer] = counted

    def handle(n, forward=True):
        hop(n).wait_recv()
        if forward:
            hop(n + parts).start()

    def loop(count, body):
        def step(i, carry):
            body(i)
            return carry

        lax.fori_loop(0, count, step, 0)

    for offset in range(1, COLUMNS):
        for copy in to_column(offset):
            copy.start()

    half = places // 2
    detour = half - FORWARD

    def next_token(more):
        pl.semaphore_wait(from_right, 1)
        pl.semaphore_wait(from_left, 1)

        @pl.when(more)
        def _():
            signal(from_right, at_place(-1))
            signal(from_left, at_place(1))

    def send_both(k):
        for copy in to_place(-k, half + k):
            copy.start()

        @pl.when(k <= FORWARD)
        def _():
            for copy in to_place(k, k):
                copy.start()

    def to_stop(j):
        there = lax.rem(place + FORWARD + 1 + j, places)
        here = pl.ds(pl.multiple_of(there * unit, unit), unit)
        return [
            pltpu.make_async_remote_copy(
                src_ref=src,
                dst_ref=dst,
                send_sem=stop_send.at[part, j],
                recv_sem=stop_recv.at[part, j],
                device_id={"seq": at_place(-STOP)},
                device_id_type=MESH,
            )
            for part, (src, dst) in enumerate(
                (
                    (along.at[here], stopped.at[pl.ds(pl.multiple_of(j * unit, unit), unit)]),
                    (tag_along.at[there], tag_stopped.at[j]),
                )
            )
        ]

    def from_stop(j):
        landing = FORWARD + 1 + j
        return [
            pltpu.make_async_remote_copy(
                src_ref=src,
                dst_ref=dst,
                send_sem=along_send.at[part, landing],
                recv_sem=along_recv.at[part, landing],
                device_id={"seq": at_place(STOP + landing - places)},
                device_id_type=MESH,
            )
            for part, (src, dst) in enumerate(
                (
                    (
                        stopped.at[pl.ds(pl.multiple_of(j * unit, unit), unit)],
                        landed.at[pl.ds(pl.multiple_of(landing * unit, unit), unit)],
                    ),
                    (tag_stopped.at[j], tag_landed.at[landing]),
                )
            )
        ]

    def early(i):
        next_token(i >= 0)
        handle(i)

    loop(STOP - 1, early)
    for offset in range(1, COLUMNS):
        for copy in to_column(offset):
            copy.wait_recv()
    row = iota((seq_count * PAGE, seq_count * PAGE), 0)
    regroup = (row % unit) // PAGE * lines + row // unit * PAGE + row % PAGE
    along[...] = jnp.dot(
        one_hot(regroup == iota((seq_count * PAGE, seq_count * PAGE), 1)),
        across[...],
        preferred_element_type=jnp.float32,
    ).astype(jnp.bfloat16)
    tag_rows = jnp.zeros((HD, seq_count), jnp.float32)
    for x in range(COLUMNS):
        mask = (iota((HD, seq_count), 0) % unit) // PAGE == x
        tag_rows = jnp.where(mask, jnp.broadcast_to(tag_across[x], (HD, seq_count)), tag_rows)
    choose = iota((places, seq_count), 1) == column * places + iota((places, seq_count), 0)
    tag_table = lax.dot_general(
        one_hot(choose),
        tag_rows.astype(jnp.bfloat16),
        (((1,), (1,)), ((), ())),
        preferred_element_type=jnp.float32,
    )
    for z in range(places):
        tag_along[z] = tag_table[z:z + 1]
    landed[pl.ds(0, unit)] = along[pl.ds(pl.multiple_of(place * unit, unit), unit)]
    tag_landed[0] = tag_along[place]
    for j in range(detour):
        for copy in to_stop(j):
            copy.start()
    loop(STOP, lambda i: send_both(i + 1))

    def late(i):
        k = i + STOP + 1
        next_token(k < half - 1)
        handle(k - 2)
        send_both(k)

    loop(half - 1 - STOP, late)
    for j in range(detour):
        for copy in to_stop(j):
            copy.wait_recv()
        for copy in from_stop(j):
            copy.start()
    done_chunks = half - 2
    pieces = kv_local * LAYERS

    def first_group(i):
        handle(done_chunks + i)
        piece(i, 0)

    loop(pieces, first_group)

    def second_group(i):
        handle(done_chunks + pieces + i)
        piece(i, GROUP)

    loop(pieces, second_group)
    last_chunks = (REACH - 1) * parts
    for n in range(done_chunks + 2 * pieces, last_chunks + 2):
        handle(n, n < last_chunks)

    def wait_pages(i):
        for copy in to_place(1, i + 1):
            copy.wait_recv()

    loop(places - 1, wait_pages)
    came = jnp.concatenate([tag_landed[z] for z in range(places)], axis=0)
    spread = jnp.dot(
        one_hot(iota((seq_count * PAGE, places), 0) // unit == iota((seq_count * PAGE, places), 1)),
        came.astype(jnp.bfloat16),
        preferred_element_type=jnp.float32,
    )
    here = iota((seq_count * PAGE, HD), 0) % unit == iota((seq_count * PAGE, HD), 1)
    tag_column = jnp.sum(jnp.where(here, spread, 0.0), axis=1, keepdims=True)
    line_column = (iota((seq_count * PAGE, 1), 0) % PAGE).astype(jnp.float32)
    lands = (tag_column - 1.0) * PAGE + line_column
    slot_lines = page_ref.shape[0]
    put = iota((seq_count * PAGE, slot_lines), 1).astype(jnp.float32) == lands
    page_ref[...] = lax.dot_general(
        one_hot(put), landed[...], (((0,), (0,)), ((), ())), preferred_element_type=jnp.float32
    ).astype(page_ref.dtype)

    def third_group(i):
        @pl.when(i < 2)
        def _():
            handle(last_chunks + 2 + i, False)

        piece(i, 2 * GROUP, True)

    loop(pieces, third_group)
    loop(REACH * parts, lambda n: hop(n).wait_send())
    for offset in range(1, COLUMNS):
        for copy in to_column(offset):
            copy.wait_send()

    def wait_sent(i):
        for copy in to_place(1, i + 1):
            copy.wait_send()

    loop(places - 1, wait_sent)
    for j in range(detour):
        for copy in to_stop(j):
            copy.wait_send()


def shards(queries, keys, values, lengths, page_owner, page_slot):
    rows = keys.shape[0]
    kv_local = keys.shape[1] // HD
    seq_count = lax.axis_size("seq")
    width = queries.shape[2]
    wide = QPER * rows
    pages_dev = rows // PAGE
    slots = pages_dev * kv_local
    places = seq_count // COLUMNS
    lines = seq_count * PAGE
    detour = places // 2 - FORWARD
    attended, pages = pl.pallas_call(
        functools.partial(ring_attention, seq_count),
        name="ring_attention",
        out_shape=(
            jax.ShapeDtypeStruct((LAYERS, rows, width), jnp.bfloat16),
            jax.ShapeDtypeStruct((slots * PAGE, 2 * HD), jnp.bfloat16),
        ),
        in_specs=[pl.BlockSpec(memory_space=pltpu.VMEM)] * 6,
        out_specs=(pl.BlockSpec(memory_space=pltpu.VMEM), pl.BlockSpec(memory_space=pltpu.VMEM)),
        scratch_shapes=[
            pltpu.VMEM((kv_local, LAYERS, wide, HD), jnp.bfloat16),
            pltpu.VMEM((2, kv_local, (REACH + 1) * rows, HD), jnp.bfloat16),
            pltpu.VMEM(((REACH + 1) * rows, rows), jnp.bfloat16),
            pltpu.VMEM((wide, rows), jnp.bfloat16),
            pltpu.VMEM((GROUP * rows, HD), jnp.bfloat16),
            pltpu.VMEM((kv_local, LAYERS, wide, HD), jnp.float32),
            pltpu.VMEM((kv_local, LAYERS, wide, HD), jnp.float32),
            pltpu.VMEM((kv_local, LAYERS, wide, HD), jnp.float32),
            pltpu.SemaphoreType.DMA((REACH * kv_local * 2,)),
            pltpu.SemaphoreType.DMA((REACH * kv_local * 2,)),
            pltpu.VMEM((lines, 2 * HD), jnp.bfloat16),
            pltpu.VMEM((lines, 2 * HD), jnp.bfloat16),
            pltpu.VMEM((lines, 2 * HD), jnp.bfloat16),
            pltpu.VMEM((lines, 2 * HD), jnp.bfloat16),
            pltpu.VMEM((COLUMNS, 1, seq_count), jnp.float32),
            pltpu.VMEM((places, 1, HD), jnp.float32),
            pltpu.VMEM((places, 1, HD), jnp.float32),
            pltpu.VMEM((detour * COLUMNS * PAGE, 2 * HD), jnp.bfloat16),
            pltpu.VMEM((detour, 1, HD), jnp.float32),
            pltpu.SemaphoreType.DMA((2, COLUMNS)),
            pltpu.SemaphoreType.DMA((2, COLUMNS)),
            pltpu.SemaphoreType.DMA((2, places)),
            pltpu.SemaphoreType.DMA((2, places)),
            pltpu.SemaphoreType.DMA((2, detour)),
            pltpu.SemaphoreType.DMA((2, detour)),
            pltpu.SemaphoreType.REGULAR,
            pltpu.SemaphoreType.REGULAR,
        ],
        compiler_params=pltpu.CompilerParams(
            collective_id=0, has_side_effects=True, vmem_limit_bytes=28 * 1024 * 1024
        ),
    )(
        queries.transpose(1, 0, 2), keys, values, lengths.reshape(1, -1),
        page_owner.transpose(1, 0), page_slot.transpose(1, 0),
    )
    return (attended.transpose(1, 0, 2), pages.reshape(slots, PAGE, 2 * HD))


def solution(mesh):
    placed = (
        P(("group", "seq"), None, "head"),
        P(("group", "seq"), "head"),
        P(("group", "seq"), "head"),
        P("group"),
        P(("group", "seq"), "head"),
        P(("group", "seq"), "head"),
    )
    return jax.shard_map(
        shards,
        mesh=mesh,
        in_specs=placed,
        out_specs=(P(("group", "seq"), None, "head"), P(("group", "seq", "head"), None, None)),
        check_vma=False,
    )
```

```python
import functools
import math

import jax
import jax.numpy as jnp
from jax import lax
from jax.experimental import pallas as pl
from jax.experimental.pallas import tpu as pltpu
from jax.sharding import PartitionSpec as P

LAYERS = 3
QPER = 5
HD = 128
PAGE = 4
REACH = 8
GROUPS = ((0, 4), (4, 3), (7, 2))
COLUMNS = 4
STOP = 8
FORWARD = 13
MESH = pl.DeviceIdType.MESH

masked_score = -16384.0
exponent_scale = math.log2(math.e) / math.sqrt(HD)


def ring_attention(
    seq_count, q_hbm, k_hbm, v_hbm, len_hbm, owner_hbm, slot_hbm, o_ref, page_ref,
    len_ref, owner_ref, slot_ref, load_sem, qs, held, bias, eye, ones, top, acc, total, send_sem, recv_sem,
    picked, across, along, landed, tag_across, tag_along, tag_landed,
    stopped, tag_stopped,
    across_send, across_recv, along_send, along_recv, stop_send, stop_recv, from_right, from_left,
):
    rows = k_hbm.shape[0]
    kv_local = held.shape[1]
    parts = 2 * kv_local
    mine = lax.axis_index("seq")
    right = lax.rem(mine + 1, seq_count)
    left = lax.rem(mine + seq_count - 1, seq_count)

    places = seq_count // COLUMNS
    column, place = mine // places, lax.rem(mine, places)

    def at_place(offset):
        return column * places + lax.rem(place + places + offset, places)

    def at_column(offset):
        return lax.rem(column + COLUMNS + offset, COLUMNS) * places + place

    def signal(sem, device):
        pl.semaphore_signal(sem, inc=1, device_id={"seq": device}, device_id_type=MESH)

    own = pl.ds(0, rows)
    pairs = [
        (ref.at[:, pl.ds(c * HD, HD)], held.at[part, c, own])
        for c in range(kv_local)
        for part, ref in enumerate((k_hbm, v_hbm))
    ]
    pairs += [(owner_hbm, owner_ref), (slot_hbm, slot_ref), (len_hbm, len_ref)]
    pairs += [
        (
            q_hbm.at[layer, :, pl.ds((c * QPER + i) * HD, HD)],
            qs.at[c, layer, pl.ds(i * rows, rows)],
        )
        for c in range(kv_local)
        for layer in range(LAYERS)
        for i in range(QPER)
    ]
    loads = [
        pltpu.make_async_copy(src, dst, load_sem.at[n]) for n, (src, dst) in enumerate(pairs)
    ]
    for load in loads:
        load.start()

    barrier = pltpu.get_barrier_semaphore()
    signal(barrier, left)
    signal(barrier, at_place(1))
    signal(barrier, at_place(-1))
    for offset in range(1, COLUMNS):
        signal(barrier, at_column(offset))
    pl.semaphore_wait(barrier, COLUMNS + 2)
    def tell(level):
        signal(from_right.at[level], at_place(-(1 << level)))
        signal(from_left.at[level], at_place(1 << level))

    def learn(level):
        pl.semaphore_wait(from_right.at[level], 1)
        pl.semaphore_wait(from_left.at[level], 1)

    def hop(n):
        slot = n // parts
        c, part = (n % parts) // 2, n % 2
        return pltpu.make_async_remote_copy(
            src_ref=held.at[part, c, pl.ds(pl.multiple_of(slot * rows, rows), rows)],
            dst_ref=held.at[part, c, pl.ds(pl.multiple_of((slot + 1) * rows, rows), rows)],
            send_sem=send_sem.at[n],
            recv_sem=recv_sem.at[n],
            device_id={"seq": right},
            device_id_type=MESH,
        )

    for n in range(parts):
        loads[n].wait()
        hop(n).start()
    tell(0)
    for load in loads[parts:parts + 3]:
        load.wait()

    lines = places * PAGE
    unit = COLUMNS * PAGE

    def iota(shape, axis):
        return lax.broadcasted_iota(jnp.int32, shape, axis)

    pages_dev = rows // PAGE
    widen = (iota((pages_dev, rows), 0) == iota((pages_dev, rows), 1) // PAGE).astype(jnp.bfloat16)

    def per_token(ref):
        wide = jnp.dot(
            ref[...].astype(jnp.float32).astype(jnp.bfloat16), widen, preferred_element_type=jnp.float32
        )
        return jnp.concatenate([wide[c:c + 1] for c in range(kv_local)], axis=1)

    owner_row = per_token(owner_ref)
    slot_row = per_token(slot_ref) + 1.0
    line_row = (iota((1, kv_local * rows), 1) % PAGE).astype(jnp.float32)
    goes = iota((seq_count * PAGE, kv_local * rows), 0).astype(jnp.float32) == owner_row * PAGE + line_row
    source = jnp.concatenate(
        [
            jnp.concatenate([held[0, c, own], held[1, c, own]], axis=1)
            for c in range(kv_local)
        ],
        axis=0,
    )

    def one_hot(mask):
        return jnp.where(mask, 1.0, 0.0).astype(jnp.bfloat16)

    picked[...] = jnp.dot(one_hot(goes), source, preferred_element_type=jnp.float32).astype(jnp.bfloat16)
    owned = (iota((seq_count, kv_local * rows), 0).astype(jnp.float32) == owner_row) & (
        jnp.broadcast_to(line_row, (seq_count, kv_local * rows)) == 0.0
    )
    tags = lax.dot_general(
        jnp.broadcast_to(slot_row, (8, kv_local * rows)).astype(jnp.bfloat16),
        one_hot(owned),
        (((1,), (1,)), ((), ())),
        preferred_element_type=jnp.float32,
    )
    tag_across[column] = tags[:1]
    own_lines = pl.ds(pl.multiple_of(column * lines, lines), lines)
    across[own_lines] = picked[own_lines]

    def to_column(offset):
        device = at_column(offset)
        first = pl.multiple_of((device // places) * lines, lines)
        return [
            pltpu.make_async_remote_copy(
                src_ref=src,
                dst_ref=dst,
                send_sem=across_send.at[part, offset],
                recv_sem=across_recv.at[part, offset],
                device_id={"seq": device},
                device_id_type=MESH,
            )
            for part, (src, dst) in enumerate(
                (
                    (picked.at[pl.ds(first, lines)], across.at[own_lines]),
                    (tag_across.at[column], tag_across.at[column]),
                )
            )
        ]

    def to_place(offset, landing):
        device = at_place(offset)
        there = lax.rem(device, places)
        return [
            pltpu.make_async_remote_copy(
                src_ref=src,
                dst_ref=dst,
                send_sem=along_send.at[part, landing],
                recv_sem=along_recv.at[part, landing],
                device_id={"seq": device},
                device_id_type=MESH,
            )
            for part, (src, dst) in enumerate(
                (
                    (
                        along.at[pl.ds(pl.multiple_of(there * unit, unit), unit)],
                        landed.at[pl.ds(pl.multiple_of(landing * unit, unit), unit)],
                    ),
                    (tag_along.at[there], tag_landed.at[landing]),
                )
            )
        ]

    learn(0)
    tell(1)

    reqs = len_ref.shape[1]
    lengths = len_ref[...].astype(jnp.float32)
    before = lax.broadcasted_iota(jnp.int32, (reqs, reqs), 1) < lax.broadcasted_iota(
        jnp.int32, (reqs, reqs), 0
    )
    starts = jnp.sum(
        jnp.where(before, jnp.broadcast_to(lengths, (reqs, reqs)), 0.0), axis=1, keepdims=True
    )
    query_pos = (mine * rows + lax.broadcasted_iota(jnp.int32, (reqs, rows), 1)).astype(jnp.float32)
    began = jnp.max(jnp.where(starts <= query_pos, starts, 0.0), axis=0, keepdims=True)
    token = (mine * rows + lax.broadcasted_iota(jnp.int32, (rows, rows), 1)).astype(jnp.float32)
    row_iota = lax.broadcasted_iota(jnp.int32, (rows, rows), 0)
    for d in range(REACH + 1):
        key_pos = ((mine - d) * rows + row_iota).astype(jnp.float32)
        allowed = (key_pos >= began) & (key_pos <= token)
        bias[pl.ds(d * rows, rows)] = jnp.where(allowed, 0.0, masked_score).astype(jnp.bfloat16)
    same = (row_iota == lax.broadcasted_iota(jnp.int32, (rows, rows), 1)).astype(jnp.bfloat16)
    for i in range(QPER):
        eye[pl.ds(i * rows, rows)] = same.astype(jnp.bfloat16)
    ones[...] = jnp.ones_like(ones)

    def piece(i, group):
        c, layer = i // LAYERS, i % LAYERS
        first, count = GROUPS[group]
        last = group == len(GROUPS) - 1
        keys = pl.ds(first * rows, count * rows)
        wide_q = jnp.concatenate([qs[c, layer], eye[...]], axis=1)
        wide_k = jnp.concatenate([held[0, c, keys], bias[keys]], axis=1)
        scores = lax.dot_general(
            wide_q, wide_k, (((1,), (1,)), ((), ())), preferred_element_type=jnp.float32
        )
        fresh = jnp.max(scores, axis=1, keepdims=True)
        if first > 0:
            old = top[c, layer]
            fresh = jnp.maximum(old, fresh)
            shrink = jnp.exp2((old - fresh) * exponent_scale)
            fresh = fresh[:, :1]
        weights = jnp.exp2((scores - fresh) * exponent_scale)
        wide_v = jnp.concatenate([held[1, c, keys], ones[pl.ds(0, count * rows)]], axis=1)
        product = jnp.dot(weights.astype(jnp.bfloat16), wide_v, preferred_element_type=jnp.float32)
        summed, counted = product[:, :HD], product[:, HD:]
        if first > 0:
            summed = acc[c, layer] * shrink + summed
            counted = total[c, layer] * shrink + counted
        if last:
            done = (summed / counted).astype(o_ref.dtype)
            for q in range(QPER):
                h = c * QPER + q
                place = h * HD if isinstance(h, int) else pl.multiple_of(h * HD, HD)
                o_ref[layer, :, pl.ds(place, HD)] = done[q * rows:(q + 1) * rows]
        else:
            top[c, layer] = jnp.broadcast_to(fresh, (QPER * rows, HD))
            acc[c, layer] = summed
            total[c, layer] = counted

    def handle(n, forward=True):
        hop(n).wait_recv()
        if forward:
            hop(n + parts).start()

    def loop(count, body):
        def step(i, carry):
            body(i)
            return carry

        lax.fori_loop(0, count, step, 0)

    for offset in range(1, COLUMNS):
        for copy in to_column(offset):
            copy.start()

    half = places // 2
    detour = half - FORWARD

    def send_both(k):
        for copy in to_place(-k, half + k):
            copy.start()

        @pl.when(k <= FORWARD)
        def _():
            for copy in to_place(k, k):
                copy.start()

    def to_stop(j):
        there = lax.rem(place + FORWARD + 1 + j, places)
        here = pl.ds(pl.multiple_of(there * unit, unit), unit)
        return [
            pltpu.make_async_remote_copy(
                src_ref=src,
                dst_ref=dst,
                send_sem=stop_send.at[part, j],
                recv_sem=stop_recv.at[part, j],
                device_id={"seq": at_place(-STOP)},
                device_id_type=MESH,
            )
            for part, (src, dst) in enumerate(
                (
                    (along.at[here], stopped.at[pl.ds(pl.multiple_of(j * unit, unit), unit)]),
                    (tag_along.at[there], tag_stopped.at[j]),
                )
            )
        ]

    def from_stop(j):
        landing = FORWARD + 1 + j
        return [
            pltpu.make_async_remote_copy(
                src_ref=src,
                dst_ref=dst,
                send_sem=along_send.at[part, landing],
                recv_sem=along_recv.at[part, landing],
                device_id={"seq": at_place(STOP + landing - places)},
                device_id_type=MESH,
            )
            for part, (src, dst) in enumerate(
                (
                    (
                        stopped.at[pl.ds(pl.multiple_of(j * unit, unit), unit)],
                        landed.at[pl.ds(pl.multiple_of(landing * unit, unit), unit)],
                    ),
                    (tag_stopped.at[j], tag_landed.at[landing]),
                )
            )
        ]

    learn(1)
    tell(2)
    loop(parts, handle)
    for offset in range(1, COLUMNS):
        for copy in to_column(offset):
            copy.wait_recv()
    row = iota((seq_count * PAGE, seq_count * PAGE), 0)
    regroup = (row % unit) // PAGE * lines + row // unit * PAGE + row % PAGE
    along[...] = jnp.dot(
        one_hot(regroup == iota((seq_count * PAGE, seq_count * PAGE), 1)),
        across[...],
        preferred_element_type=jnp.float32,
    ).astype(jnp.bfloat16)
    tag_rows = jnp.zeros((HD, seq_count), jnp.float32)
    for x in range(COLUMNS):
        mask = (iota((HD, seq_count), 0) % unit) // PAGE == x
        tag_rows = jnp.where(mask, jnp.broadcast_to(tag_across[x], (HD, seq_count)), tag_rows)
    choose = iota((places, seq_count), 1) == column * places + iota((places, seq_count), 0)
    tag_table = lax.dot_general(
        one_hot(choose),
        tag_rows.astype(jnp.bfloat16),
        (((1,), (1,)), ((), ())),
        preferred_element_type=jnp.float32,
    )
    for z in range(places):
        tag_along[z] = tag_table[z:z + 1]
    landed[pl.ds(0, unit)] = along[pl.ds(pl.multiple_of(place * unit, unit), unit)]
    tag_landed[0] = tag_along[place]
    learn(2)
    tell(3)
    for j in range(detour):
        for copy in to_stop(j):
            copy.start()
    loop(STOP, lambda i: send_both(i + 1))

    loop(2 * parts, lambda i: handle(parts + i))
    for load in loads[parts + 3:]:
        load.wait()
    learn(3)
    loop(half - 1 - STOP, lambda i: send_both(STOP + 1 + i))
    pieces = kv_local * LAYERS

    def first_group(i):
        handle(3 * parts + 2 * i)
        piece(i, 0)
        handle(3 * parts + 1 + 2 * i)

    loop(pieces, first_group)
    for j in range(detour):
        for copy in to_stop(j):
            copy.wait_recv()
        for copy in from_stop(j):
            copy.start()
    next_chunk = 3 * parts + 2 * pieces
    last_chunks = (REACH - 1) * parts

    def second_group(i):
        n = next_chunk + i
        hop(n).wait_recv()

        @pl.when(n < last_chunks)
        def _():
            hop(n + parts).start()

        piece(i, 1)

    loop(pieces, second_group)

    def wait_pages(i):
        for copy in to_place(1, i + 1):
            copy.wait_recv()

    loop(places - 1, wait_pages)
    came = jnp.concatenate([tag_landed[z] for z in range(places)], axis=0)
    spread = jnp.dot(
        one_hot(iota((seq_count * PAGE, places), 0) // unit == iota((seq_count * PAGE, places), 1)),
        came.astype(jnp.bfloat16),
        preferred_element_type=jnp.float32,
    )
    here = iota((seq_count * PAGE, HD), 0) % unit == iota((seq_count * PAGE, HD), 1)
    tag_column = jnp.sum(jnp.where(here, spread, 0.0), axis=1, keepdims=True)
    line_column = (iota((seq_count * PAGE, 1), 0) % PAGE).astype(jnp.float32)
    lands = (tag_column - 1.0) * PAGE + line_column
    slot_lines = page_ref.shape[0]
    put = iota((seq_count * PAGE, slot_lines), 1).astype(jnp.float32) == lands
    page_ref[...] = lax.dot_general(
        one_hot(put), landed[...], (((0,), (0,)), ((), ())), preferred_element_type=jnp.float32
    ).astype(page_ref.dtype)

    def third_group(i):
        @pl.when(i < REACH * parts - next_chunk - pieces)
        def _():
            handle(next_chunk + pieces + i, False)

        piece(i, 2)

    loop(pieces, third_group)
    loop(REACH * parts, lambda n: hop(n).wait_send())
    for offset in range(1, COLUMNS):
        for copy in to_column(offset):
            copy.wait_send()

    def wait_sent(i):
        for copy in to_place(1, i + 1):
            copy.wait_send()

    loop(places - 1, wait_sent)
    for j in range(detour):
        for copy in to_stop(j):
            copy.wait_send()


def shards(queries, keys, values, lengths, page_owner, page_slot):
    rows = keys.shape[0]
    kv_local = keys.shape[1] // HD
    seq_count = lax.axis_size("seq")
    width = queries.shape[2]
    wide = QPER * rows
    pages_dev = rows // PAGE
    slots = pages_dev * kv_local
    places = seq_count // COLUMNS
    lines = seq_count * PAGE
    detour = places // 2 - FORWARD
    attended, pages = pl.pallas_call(
        functools.partial(ring_attention, seq_count),
        name="ring_attention",
        out_shape=(
            jax.ShapeDtypeStruct((LAYERS, rows, width), jnp.bfloat16),
            jax.ShapeDtypeStruct((slots * PAGE, 2 * HD), jnp.bfloat16),
        ),
        in_specs=[pl.BlockSpec(memory_space=pltpu.HBM)] * 6,
        out_specs=(pl.BlockSpec(memory_space=pltpu.VMEM), pl.BlockSpec(memory_space=pltpu.VMEM)),
        scratch_shapes=[
            pltpu.VMEM((1, lengths.shape[0]), jnp.int32),
            pltpu.VMEM((kv_local, pages_dev), jnp.int32),
            pltpu.VMEM((kv_local, pages_dev), jnp.int32),
            pltpu.SemaphoreType.DMA((2 * kv_local + 3 + kv_local * LAYERS * QPER,)),
            pltpu.VMEM((kv_local, LAYERS, wide, HD), jnp.bfloat16),
            pltpu.VMEM((2, kv_local, (REACH + 1) * rows, HD), jnp.bfloat16),
            pltpu.VMEM(((REACH + 1) * rows, rows), jnp.bfloat16),
            pltpu.VMEM((wide, rows), jnp.bfloat16),
            pltpu.VMEM((max(count for _, count in GROUPS) * rows, HD), jnp.bfloat16),
            pltpu.VMEM((kv_local, LAYERS, wide, HD), jnp.float32),
            pltpu.VMEM((kv_local, LAYERS, wide, HD), jnp.float32),
            pltpu.VMEM((kv_local, LAYERS, wide, HD), jnp.float32),
            pltpu.SemaphoreType.DMA((REACH * kv_local * 2,)),
            pltpu.SemaphoreType.DMA((REACH * kv_local * 2,)),
            pltpu.VMEM((lines, 2 * HD), jnp.bfloat16),
            pltpu.VMEM((lines, 2 * HD), jnp.bfloat16),
            pltpu.VMEM((lines, 2 * HD), jnp.bfloat16),
            pltpu.VMEM((lines, 2 * HD), jnp.bfloat16),
            pltpu.VMEM((COLUMNS, 1, seq_count), jnp.float32),
            pltpu.VMEM((places, 1, HD), jnp.float32),
            pltpu.VMEM((places, 1, HD), jnp.float32),
            pltpu.VMEM((detour * COLUMNS * PAGE, 2 * HD), jnp.bfloat16),
            pltpu.VMEM((detour, 1, HD), jnp.float32),
            pltpu.SemaphoreType.DMA((2, COLUMNS)),
            pltpu.SemaphoreType.DMA((2, COLUMNS)),
            pltpu.SemaphoreType.DMA((2, places)),
            pltpu.SemaphoreType.DMA((2, places)),
            pltpu.SemaphoreType.DMA((2, detour)),
            pltpu.SemaphoreType.DMA((2, detour)),
            pltpu.SemaphoreType.REGULAR((4,)),
            pltpu.SemaphoreType.REGULAR((4,)),
        ],
        compiler_params=pltpu.CompilerParams(
            collective_id=0, has_side_effects=True, vmem_limit_bytes=28 * 1024 * 1024
        ),
    )(
        *(
            pltpu.with_memory_space_constraint(x, pltpu.HBM)
            for x in (
                queries.transpose(1, 0, 2), keys, values, lengths.reshape(1, -1),
                page_owner.transpose(1, 0), page_slot.transpose(1, 0),
            )
        )
    )
    return (attended.transpose(1, 0, 2), pages.reshape(slots, PAGE, 2 * HD))


def solution(mesh):
    placed = (
        P(("group", "seq"), None, "head"),
        P(("group", "seq"), "head"),
        P(("group", "seq"), "head"),
        P("group"),
        P(("group", "seq"), "head"),
        P(("group", "seq"), "head"),
    )
    return jax.shard_map(
        shards,
        mesh=mesh,
        in_specs=placed,
        out_specs=(P(("group", "seq"), None, "head"), P(("group", "seq", "head"), None, None)),
        check_vma=False,
    )
```

```python
import functools
import math

import jax
import jax.numpy as jnp
from jax import lax
from jax.experimental import pallas as pl
from jax.experimental.pallas import tpu as pltpu
from jax.sharding import PartitionSpec as P

LAYERS = 3
QPER = 5
HD = 128
PAGE = 4
REACH = 8
GROUPS = ((0, 2), (2, 2), (4, 2), (6, 3))
COLUMNS = 4
STOP = 8
FORWARD = 12
NEAR = 4
MESH = pl.DeviceIdType.MESH

masked_score = -16384.0
exponent_scale = math.log2(math.e) / math.sqrt(HD)


def ring_attention(
    seq_count, q_hbm, k_hbm, v_hbm, len_hbm, owner_hbm, slot_hbm, o_ref, page_ref,
    len_ref, owner_ref, slot_ref, load_sem, qs, held, bias, eye, ones, top, acc, total, send_sem, recv_sem,
    picked, across, along, landed, tag_across, tag_along, tag_landed,
    stopped, tag_stopped,
    across_send, across_recv, along_send, along_recv, stop_send, stop_recv, from_right, from_left,
):
    rows = k_hbm.shape[0]
    kv_local = held.shape[1]
    parts = 2 * kv_local
    mine = lax.axis_index("seq")
    right = lax.rem(mine + 1, seq_count)
    left = lax.rem(mine + seq_count - 1, seq_count)

    places = seq_count // COLUMNS
    column, place = mine // places, lax.rem(mine, places)

    def at_place(offset):
        return column * places + lax.rem(place + places + offset, places)

    def at_column(offset):
        return lax.rem(column + COLUMNS + offset, COLUMNS) * places + place

    def signal(sem, device):
        pl.semaphore_signal(sem, inc=1, device_id={"seq": device}, device_id_type=MESH)

    own = pl.ds(0, rows)
    pairs = [
        (ref.at[:, pl.ds(c * HD, HD)], held.at[part, c, own])
        for c in range(kv_local)
        for part, ref in enumerate((k_hbm, v_hbm))
    ]
    pairs += [(owner_hbm, owner_ref), (slot_hbm, slot_ref), (len_hbm, len_ref)]
    pairs += [
        (
            q_hbm.at[layer, :, pl.ds((c * QPER + i) * HD, HD)],
            qs.at[c, layer, pl.ds(i * rows, rows)],
        )
        for c in range(kv_local)
        for layer in range(LAYERS)
        for i in range(QPER)
    ]
    loads = [
        pltpu.make_async_copy(src, dst, load_sem.at[n]) for n, (src, dst) in enumerate(pairs)
    ]
    for load in loads:
        load.start()

    barrier = pltpu.get_barrier_semaphore()
    signal(barrier, left)
    signal(barrier, at_place(1))
    signal(barrier, at_place(-1))
    for offset in range(1, COLUMNS):
        signal(barrier, at_column(offset))
    pl.semaphore_wait(barrier, COLUMNS + 2)
    def tell(level):
        signal(from_right.at[level], at_place(-(1 << level)))
        signal(from_left.at[level], at_place(1 << level))

    def learn(level):
        pl.semaphore_wait(from_right.at[level], 1)
        pl.semaphore_wait(from_left.at[level], 1)

    def hop(n):
        slot = n // parts
        c, part = (n % parts) // 2, n % 2
        return pltpu.make_async_remote_copy(
            src_ref=held.at[part, c, pl.ds(pl.multiple_of(slot * rows, rows), rows)],
            dst_ref=held.at[part, c, pl.ds(pl.multiple_of((slot + 1) * rows, rows), rows)],
            send_sem=send_sem.at[n],
            recv_sem=recv_sem.at[n],
            device_id={"seq": right},
            device_id_type=MESH,
        )

    for n in range(parts):
        loads[n].wait()
        hop(n).start()
    tell(0)
    for load in loads[parts:parts + 3]:
        load.wait()

    lines = places * PAGE
    unit = COLUMNS * PAGE

    def iota(shape, axis):
        return lax.broadcasted_iota(jnp.int32, shape, axis)

    pages_dev = rows // PAGE
    widen = (iota((pages_dev, rows), 0) == iota((pages_dev, rows), 1) // PAGE).astype(jnp.bfloat16)

    def per_token(ref):
        wide = jnp.dot(
            ref[...].astype(jnp.float32).astype(jnp.bfloat16), widen, preferred_element_type=jnp.float32
        )
        return jnp.concatenate([wide[c:c + 1] for c in range(kv_local)], axis=1)

    owner_row = per_token(owner_ref)
    slot_row = per_token(slot_ref) + 1.0
    line_row = (iota((1, kv_local * rows), 1) % PAGE).astype(jnp.float32)
    goes = iota((seq_count * PAGE, kv_local * rows), 0).astype(jnp.float32) == owner_row * PAGE + line_row
    source = jnp.concatenate(
        [
            jnp.concatenate([held[0, c, own], held[1, c, own]], axis=1)
            for c in range(kv_local)
        ],
        axis=0,
    )

    def one_hot(mask):
        return jnp.where(mask, 1.0, 0.0).astype(jnp.bfloat16)

    picked[...] = jnp.dot(one_hot(goes), source, preferred_element_type=jnp.float32).astype(jnp.bfloat16)
    owned = (iota((seq_count, kv_local * rows), 0).astype(jnp.float32) == owner_row) & (
        jnp.broadcast_to(line_row, (seq_count, kv_local * rows)) == 0.0
    )
    tags = lax.dot_general(
        jnp.broadcast_to(slot_row, (8, kv_local * rows)).astype(jnp.bfloat16),
        one_hot(owned),
        (((1,), (1,)), ((), ())),
        preferred_element_type=jnp.float32,
    )
    tag_across[column] = tags[:1]
    own_lines = pl.ds(pl.multiple_of(column * lines, lines), lines)
    across[own_lines] = picked[own_lines]

    def to_column(offset):
        device = at_column(offset)
        first = pl.multiple_of((device // places) * lines, lines)
        return [
            pltpu.make_async_remote_copy(
                src_ref=src,
                dst_ref=dst,
                send_sem=across_send.at[part, offset],
                recv_sem=across_recv.at[part, offset],
                device_id={"seq": device},
                device_id_type=MESH,
            )
            for part, (src, dst) in enumerate(
                (
                    (picked.at[pl.ds(first, lines)], across.at[own_lines]),
                    (tag_across.at[column], tag_across.at[column]),
                )
            )
        ]

    def to_place(offset, landing):
        device = at_place(offset)
        there = lax.rem(device, places)
        return [
            pltpu.make_async_remote_copy(
                src_ref=src,
                dst_ref=dst,
                send_sem=along_send.at[part, landing],
                recv_sem=along_recv.at[part, landing],
                device_id={"seq": device},
                device_id_type=MESH,
            )
            for part, (src, dst) in enumerate(
                (
                    (
                        along.at[pl.ds(pl.multiple_of(there * unit, unit), unit)],
                        landed.at[pl.ds(pl.multiple_of(landing * unit, unit), unit)],
                    ),
                    (tag_along.at[there], tag_landed.at[landing]),
                )
            )
        ]

    reqs = len_ref.shape[1]
    lengths = len_ref[...].astype(jnp.float32)
    before = lax.broadcasted_iota(jnp.int32, (reqs, reqs), 1) < lax.broadcasted_iota(
        jnp.int32, (reqs, reqs), 0
    )
    starts = jnp.sum(
        jnp.where(before, jnp.broadcast_to(lengths, (reqs, reqs)), 0.0), axis=1, keepdims=True
    )
    query_pos = (mine * rows + lax.broadcasted_iota(jnp.int32, (reqs, rows), 1)).astype(jnp.float32)
    began = jnp.max(jnp.where(starts <= query_pos, starts, 0.0), axis=0, keepdims=True)
    token = (mine * rows + lax.broadcasted_iota(jnp.int32, (rows, rows), 1)).astype(jnp.float32)
    row_iota = lax.broadcasted_iota(jnp.int32, (rows, rows), 0)
    for d in range(REACH + 1):
        key_pos = ((mine - d) * rows + row_iota).astype(jnp.float32)
        allowed = (key_pos >= began) & (key_pos <= token)
        bias[pl.ds(d * rows, rows)] = jnp.where(allowed, 0.0, masked_score).astype(jnp.bfloat16)
    same = (row_iota == lax.broadcasted_iota(jnp.int32, (rows, rows), 1)).astype(jnp.bfloat16)
    for i in range(QPER):
        eye[pl.ds(i * rows, rows)] = same.astype(jnp.bfloat16)
    ones[...] = jnp.ones_like(ones)
    for offset in range(1, COLUMNS):
        for copy in to_column(offset):
            copy.start()
    learn(0)
    tell(1)

    def piece(i, group):
        c, layer = i // LAYERS, i % LAYERS
        first, count = GROUPS[group]
        last = group == len(GROUPS) - 1
        keys = pl.ds(first * rows, count * rows)
        wide_q = jnp.concatenate([qs[c, layer], eye[...]], axis=1)
        wide_k = jnp.concatenate([held[0, c, keys], bias[keys]], axis=1)
        scores = lax.dot_general(
            wide_q, wide_k, (((1,), (1,)), ((), ())), preferred_element_type=jnp.float32
        )
        fresh = jnp.max(scores, axis=1, keepdims=True)
        if first > 0:
            old = top[c, layer]
            fresh = jnp.maximum(old, fresh)
            shrink = jnp.exp2((old - fresh) * exponent_scale)
            fresh = fresh[:, :1]
        weights = jnp.exp2((scores - fresh) * exponent_scale)
        wide_v = jnp.concatenate([held[1, c, keys], ones[pl.ds(0, count * rows)]], axis=1)
        product = jnp.dot(weights.astype(jnp.bfloat16), wide_v, preferred_element_type=jnp.float32)
        summed, counted = product[:, :HD], product[:, HD:]
        if first > 0:
            summed = acc[c, layer] * shrink + summed
            counted = total[c, layer] * shrink + counted
        if last:
            done = (summed / counted).astype(o_ref.dtype)
            for q in range(QPER):
                h = c * QPER + q
                place = h * HD if isinstance(h, int) else pl.multiple_of(h * HD, HD)
                o_ref[layer, :, pl.ds(place, HD)] = done[q * rows:(q + 1) * rows]
        else:
            top[c, layer] = jnp.broadcast_to(fresh, (QPER * rows, HD))
            acc[c, layer] = summed
            total[c, layer] = counted

    def handle(n, forward=True):
        hop(n).wait_recv()
        if forward:
            hop(n + parts).start()

    def loop(count, body):
        def step(i, carry):
            body(i)
            return carry

        lax.fori_loop(0, count, step, 0)

    half = places // 2
    detour = half - FORWARD

    def send_both(k):
        for copy in to_place(-k, half + k):
            copy.start()

        @pl.when(k <= FORWARD)
        def _():
            for copy in to_place(k, k):
                copy.start()

    def to_stop(j):
        there = lax.rem(place + FORWARD + 1 + j, places)
        here = pl.ds(pl.multiple_of(there * unit, unit), unit)
        return [
            pltpu.make_async_remote_copy(
                src_ref=src,
                dst_ref=dst,
                send_sem=stop_send.at[part, j],
                recv_sem=stop_recv.at[part, j],
                device_id={"seq": at_place(-STOP)},
                device_id_type=MESH,
            )
            for part, (src, dst) in enumerate(
                (
                    (along.at[here], stopped.at[pl.ds(pl.multiple_of(j * unit, unit), unit)]),
                    (tag_along.at[there], tag_stopped.at[j]),
                )
            )
        ]

    def from_stop(j):
        landing = FORWARD + 1 + j
        return [
            pltpu.make_async_remote_copy(
                src_ref=src,
                dst_ref=dst,
                send_sem=along_send.at[part, landing],
                recv_sem=along_recv.at[part, landing],
                device_id={"seq": at_place(STOP + landing - places)},
                device_id_type=MESH,
            )
            for part, (src, dst) in enumerate(
                (
                    (
                        stopped.at[pl.ds(pl.multiple_of(j * unit, unit), unit)],
                        landed.at[pl.ds(pl.multiple_of(landing * unit, unit), unit)],
                    ),
                    (tag_stopped.at[j], tag_landed.at[landing]),
                )
            )
        ]

    learn(1)
    tell(2)
    loop(parts, handle)
    for offset in range(1, COLUMNS):
        for copy in to_column(offset):
            copy.wait_recv()
    row = iota((seq_count * PAGE, seq_count * PAGE), 0)
    regroup = (row % unit) // PAGE * lines + row // unit * PAGE + row % PAGE
    along[...] = jnp.dot(
        one_hot(regroup == iota((seq_count * PAGE, seq_count * PAGE), 1)),
        across[...],
        preferred_element_type=jnp.float32,
    ).astype(jnp.bfloat16)
    tag_rows = jnp.zeros((HD, seq_count), jnp.float32)
    for x in range(COLUMNS):
        mask = (iota((HD, seq_count), 0) % unit) // PAGE == x
        tag_rows = jnp.where(mask, jnp.broadcast_to(tag_across[x], (HD, seq_count)), tag_rows)
    choose = iota((places, seq_count), 1) == column * places + iota((places, seq_count), 0)
    tag_table = lax.dot_general(
        one_hot(choose),
        tag_rows.astype(jnp.bfloat16),
        (((1,), (1,)), ((), ())),
        preferred_element_type=jnp.float32,
    )
    for z in range(places):
        tag_along[z] = tag_table[z:z + 1]
    landed[pl.ds(0, unit)] = along[pl.ds(pl.multiple_of(place * unit, unit), unit)]
    tag_landed[0] = tag_along[place]
    loop(NEAR, lambda i: send_both(i + 1))
    learn(2)
    tell(3)
    for j in range(detour):
        for copy in to_stop(j):
            copy.start()
    loop(STOP - NEAR, lambda i: send_both(NEAR + 1 + i))

    for load in loads[parts + 3:]:
        load.wait()
    pieces = kv_local * LAYERS
    last_chunks = (REACH - 1) * parts

    def beside(group):
        first_chunk = (GROUPS[group][0] + 1) * parts

        def step(i):
            handle(first_chunk + i)
            piece(i, group)

        loop(pieces, step)
        for n in range(first_chunk + pieces, first_chunk + 2 * parts):
            handle(n)

    beside(0)
    learn(3)
    loop(half - 1 - STOP, lambda i: send_both(STOP + 1 + i))
    beside(1)
    for j in range(detour):
        for copy in to_stop(j):
            copy.wait_recv()
        for copy in from_stop(j):
            copy.start()
    beside(2)
    for n in range(last_chunks, last_chunks + 2):
        handle(n, False)

    def last_group(i):
        @pl.when(i < 2)
        def _():
            handle(last_chunks + 2 + i, False)

        piece(i, 3)

    loop(pieces, last_group)

    def wait_pages(i):
        for copy in to_place(1, i + 1):
            copy.wait_recv()

    loop(places - 1, wait_pages)
    came = jnp.concatenate([tag_landed[z] for z in range(places)], axis=0)
    spread = jnp.dot(
        one_hot(iota((seq_count * PAGE, places), 0) // unit == iota((seq_count * PAGE, places), 1)),
        came.astype(jnp.bfloat16),
        preferred_element_type=jnp.float32,
    )
    here = iota((seq_count * PAGE, HD), 0) % unit == iota((seq_count * PAGE, HD), 1)
    tag_column = jnp.sum(jnp.where(here, spread, 0.0), axis=1, keepdims=True)
    line_column = (iota((seq_count * PAGE, 1), 0) % PAGE).astype(jnp.float32)
    lands = (tag_column - 1.0) * PAGE + line_column
    slot_lines = page_ref.shape[0]
    put = iota((seq_count * PAGE, slot_lines), 1).astype(jnp.float32) == lands
    page_ref[...] = lax.dot_general(
        one_hot(put), landed[...], (((0,), (0,)), ((), ())), preferred_element_type=jnp.float32
    ).astype(page_ref.dtype)

    loop(REACH * parts, lambda n: hop(n).wait_send())
    for offset in range(1, COLUMNS):
        for copy in to_column(offset):
            copy.wait_send()

    def wait_sent(i):
        for copy in to_place(1, i + 1):
            copy.wait_send()

    loop(places - 1, wait_sent)
    for j in range(detour):
        for copy in to_stop(j):
            copy.wait_send()


def shards(queries, keys, values, lengths, page_owner, page_slot):
    rows = keys.shape[0]
    kv_local = keys.shape[1] // HD
    seq_count = lax.axis_size("seq")
    width = queries.shape[2]
    wide = QPER * rows
    pages_dev = rows // PAGE
    slots = pages_dev * kv_local
    places = seq_count // COLUMNS
    lines = seq_count * PAGE
    detour = places // 2 - FORWARD
    attended, pages = pl.pallas_call(
        functools.partial(ring_attention, seq_count),
        name="ring_attention",
        out_shape=(
            jax.ShapeDtypeStruct((LAYERS, rows, width), jnp.bfloat16),
            jax.ShapeDtypeStruct((slots * PAGE, 2 * HD), jnp.bfloat16),
        ),
        in_specs=[pl.BlockSpec(memory_space=pltpu.HBM)] * 6,
        out_specs=(pl.BlockSpec(memory_space=pltpu.VMEM), pl.BlockSpec(memory_space=pltpu.VMEM)),
        scratch_shapes=[
            pltpu.VMEM((1, lengths.shape[0]), jnp.int32),
            pltpu.VMEM((kv_local, pages_dev), jnp.int32),
            pltpu.VMEM((kv_local, pages_dev), jnp.int32),
            pltpu.SemaphoreType.DMA((2 * kv_local + 3 + kv_local * LAYERS * QPER,)),
            pltpu.VMEM((kv_local, LAYERS, wide, HD), jnp.bfloat16),
            pltpu.VMEM((2, kv_local, (REACH + 1) * rows, HD), jnp.bfloat16),
            pltpu.VMEM(((REACH + 1) * rows, rows), jnp.bfloat16),
            pltpu.VMEM((wide, rows), jnp.bfloat16),
            pltpu.VMEM((max(count for _, count in GROUPS) * rows, HD), jnp.bfloat16),
            pltpu.VMEM((kv_local, LAYERS, wide, HD), jnp.float32),
            pltpu.VMEM((kv_local, LAYERS, wide, HD), jnp.float32),
            pltpu.VMEM((kv_local, LAYERS, wide, HD), jnp.float32),
            pltpu.SemaphoreType.DMA((REACH * kv_local * 2,)),
            pltpu.SemaphoreType.DMA((REACH * kv_local * 2,)),
            pltpu.VMEM((lines, 2 * HD), jnp.bfloat16),
            pltpu.VMEM((lines, 2 * HD), jnp.bfloat16),
            pltpu.VMEM((lines, 2 * HD), jnp.bfloat16),
            pltpu.VMEM((lines, 2 * HD), jnp.bfloat16),
            pltpu.VMEM((COLUMNS, 1, seq_count), jnp.float32),
            pltpu.VMEM((places, 1, HD), jnp.float32),
            pltpu.VMEM((places, 1, HD), jnp.float32),
            pltpu.VMEM((detour * COLUMNS * PAGE, 2 * HD), jnp.bfloat16),
            pltpu.VMEM((detour, 1, HD), jnp.float32),
            pltpu.SemaphoreType.DMA((2, COLUMNS)),
            pltpu.SemaphoreType.DMA((2, COLUMNS)),
            pltpu.SemaphoreType.DMA((2, places)),
            pltpu.SemaphoreType.DMA((2, places)),
            pltpu.SemaphoreType.DMA((2, detour)),
            pltpu.SemaphoreType.DMA((2, detour)),
            pltpu.SemaphoreType.REGULAR((4,)),
            pltpu.SemaphoreType.REGULAR((4,)),
        ],
        compiler_params=pltpu.CompilerParams(
            collective_id=0, has_side_effects=True, vmem_limit_bytes=28 * 1024 * 1024
        ),
    )(
        *(
            pltpu.with_memory_space_constraint(x, pltpu.HBM)
            for x in (
                queries.transpose(1, 0, 2), keys, values, lengths.reshape(1, -1),
                page_owner.transpose(1, 0), page_slot.transpose(1, 0),
            )
        )
    )
    return (attended.transpose(1, 0, 2), pages.reshape(slots, PAGE, 2 * HD))


def solution(mesh):
    placed = (
        P(("group", "seq"), None, "head"),
        P(("group", "seq"), "head"),
        P(("group", "seq"), "head"),
        P("group"),
        P(("group", "seq"), "head"),
        P(("group", "seq"), "head"),
    )
    return jax.shard_map(
        shards,
        mesh=mesh,
        in_specs=placed,
        out_specs=(P(("group", "seq"), None, "head"), P(("group", "seq", "head"), None, None)),
        check_vma=False,
    )
```

```python
import functools
import math

import jax
import jax.numpy as jnp
from jax import lax
from jax.experimental import pallas as pl
from jax.experimental.pallas import tpu as pltpu
from jax.sharding import PartitionSpec as P

LAYERS = 3
QPER = 5
HD = 128
PAGE = 4
REACH = 8
GROUPS = ((0, 2), (2, 2), (4, 2), (6, 3))
COLUMNS = 4
STOP = 8
FORWARD = 12
NEAR = 4
MESH = pl.DeviceIdType.MESH

masked_score = -16384.0
exponent_scale = math.log2(math.e) / math.sqrt(HD)


def ring_attention(
    seq_count, q_hbm, k_hbm, v_hbm, len_hbm, owner_hbm, slot_hbm, o_ref, page_ref,
    len_ref, owner_ref, slot_ref, load_sem, qs, held, bias, eye, ones, top, acc, total, send_sem, recv_sem,
    picked, across, along, landed, tag_across, tag_along, tag_landed,
    stopped, tag_stopped,
    across_send, across_recv, along_send, along_recv, stop_send, stop_recv, from_right, from_left,
):
    rows = k_hbm.shape[0]
    kv_local = held.shape[1]
    parts = 2 * kv_local
    mine = lax.axis_index("seq")
    right = lax.rem(mine + 1, seq_count)
    left = lax.rem(mine + seq_count - 1, seq_count)

    places = seq_count // COLUMNS
    column, place = mine // places, lax.rem(mine, places)

    def at_place(offset):
        return column * places + lax.rem(place + places + offset, places)

    def at_column(offset):
        return lax.rem(column + COLUMNS + offset, COLUMNS) * places + place

    def signal(sem, device):
        pl.semaphore_signal(sem, inc=1, device_id={"seq": device}, device_id_type=MESH)

    own = pl.ds(0, rows)
    pairs = [
        (ref.at[:, pl.ds(c * HD, HD)], held.at[part, c, own])
        for c in range(kv_local)
        for part, ref in enumerate((k_hbm, v_hbm))
    ]
    pairs += [(owner_hbm, owner_ref), (slot_hbm, slot_ref), (len_hbm, len_ref)]
    pairs += [
        (
            q_hbm.at[layer, :, pl.ds((c * QPER + i) * HD, HD)],
            qs.at[c, layer, pl.ds(i * rows, rows)],
        )
        for c in range(kv_local)
        for layer in range(LAYERS)
        for i in range(QPER)
    ]
    loads = [
        pltpu.make_async_copy(src, dst, load_sem.at[n]) for n, (src, dst) in enumerate(pairs)
    ]
    for load in loads:
        load.start()

    barrier = pltpu.get_barrier_semaphore()
    signal(barrier, left)
    signal(barrier, at_place(1))
    signal(barrier, at_place(-1))
    for offset in range(1, COLUMNS):
        signal(barrier, at_column(offset))
    pl.semaphore_wait(barrier, COLUMNS + 2)
    def tell(level):
        signal(from_right.at[level], at_place(-(1 << level)))
        signal(from_left.at[level], at_place(1 << level))

    def learn(level):
        pl.semaphore_wait(from_right.at[level], 1)
        pl.semaphore_wait(from_left.at[level], 1)

    def hop(n):
        slot = n // parts
        c, part = (n % parts) // 2, n % 2
        return pltpu.make_async_remote_copy(
            src_ref=held.at[part, c, pl.ds(pl.multiple_of(slot * rows, rows), rows)],
            dst_ref=held.at[part, c, pl.ds(pl.multiple_of((slot + 1) * rows, rows), rows)],
            send_sem=send_sem.at[n],
            recv_sem=recv_sem.at[n],
            device_id={"seq": right},
            device_id_type=MESH,
        )

    for n in range(parts):
        loads[n].wait()
        hop(n).start()
    tell(0)
    for load in loads[parts:parts + 3]:
        load.wait()

    lines = places * PAGE
    unit = COLUMNS * PAGE

    def iota(shape, axis):
        return lax.broadcasted_iota(jnp.int32, shape, axis)

    pages_dev = rows // PAGE
    widen = (iota((pages_dev, rows), 0) == iota((pages_dev, rows), 1) // PAGE).astype(jnp.bfloat16)

    def per_token(ref):
        wide = jnp.dot(
            ref[...].astype(jnp.float32).astype(jnp.bfloat16), widen, preferred_element_type=jnp.float32
        )
        return jnp.concatenate([wide[c:c + 1] for c in range(kv_local)], axis=1)

    owner_row = per_token(owner_ref)
    slot_row = per_token(slot_ref) + 1.0
    line_row = (iota((1, kv_local * rows), 1) % PAGE).astype(jnp.float32)
    goes = iota((seq_count * PAGE, kv_local * rows), 0).astype(jnp.float32) == owner_row * PAGE + line_row
    source = jnp.concatenate(
        [
            jnp.concatenate([held[0, c, own], held[1, c, own]], axis=1)
            for c in range(kv_local)
        ],
        axis=0,
    )

    def one_hot(mask):
        return jnp.where(mask, 1.0, 0.0).astype(jnp.bfloat16)

    picked[...] = jnp.dot(one_hot(goes), source, preferred_element_type=jnp.float32).astype(jnp.bfloat16)
    owned = (iota((seq_count, kv_local * rows), 0).astype(jnp.float32) == owner_row) & (
        jnp.broadcast_to(line_row, (seq_count, kv_local * rows)) == 0.0
    )
    tags = lax.dot_general(
        jnp.broadcast_to(slot_row, (8, kv_local * rows)).astype(jnp.bfloat16),
        one_hot(owned),
        (((1,), (1,)), ((), ())),
        preferred_element_type=jnp.float32,
    )
    tag_across[column] = tags[:1]
    own_lines = pl.ds(pl.multiple_of(column * lines, lines), lines)
    across[own_lines] = picked[own_lines]

    def to_column(offset):
        device = at_column(offset)
        first = pl.multiple_of((device // places) * lines, lines)
        return [
            pltpu.make_async_remote_copy(
                src_ref=src,
                dst_ref=dst,
                send_sem=across_send.at[part, offset],
                recv_sem=across_recv.at[part, offset],
                device_id={"seq": device},
                device_id_type=MESH,
            )
            for part, (src, dst) in enumerate(
                (
                    (picked.at[pl.ds(first, lines)], across.at[own_lines]),
                    (tag_across.at[column], tag_across.at[column]),
                )
            )
        ]

    def to_place(offset, landing):
        device = at_place(offset)
        there = lax.rem(device, places)
        return [
            pltpu.make_async_remote_copy(
                src_ref=src,
                dst_ref=dst,
                send_sem=along_send.at[part, landing],
                recv_sem=along_recv.at[part, landing],
                device_id={"seq": device},
                device_id_type=MESH,
            )
            for part, (src, dst) in enumerate(
                (
                    (
                        along.at[pl.ds(pl.multiple_of(there * unit, unit), unit)],
                        landed.at[pl.ds(pl.multiple_of(landing * unit, unit), unit)],
                    ),
                    (tag_along.at[there], tag_landed.at[landing]),
                )
            )
        ]

    reqs = len_ref.shape[1]
    lengths = len_ref[...].astype(jnp.float32)
    before = lax.broadcasted_iota(jnp.int32, (reqs, reqs), 1) < lax.broadcasted_iota(
        jnp.int32, (reqs, reqs), 0
    )
    starts = jnp.sum(
        jnp.where(before, jnp.broadcast_to(lengths, (reqs, reqs)), 0.0), axis=1, keepdims=True
    )
    query_pos = (mine * rows + lax.broadcasted_iota(jnp.int32, (reqs, rows), 1)).astype(jnp.float32)
    began = jnp.max(jnp.where(starts <= query_pos, starts, 0.0), axis=0, keepdims=True)
    token = (mine * rows + lax.broadcasted_iota(jnp.int32, (rows, rows), 1)).astype(jnp.float32)
    row_iota = lax.broadcasted_iota(jnp.int32, (rows, rows), 0)
    for d in range(REACH + 1):
        key_pos = ((mine - d) * rows + row_iota).astype(jnp.float32)
        allowed = (key_pos >= began) & (key_pos <= token)
        bias[pl.ds(d * rows, rows)] = jnp.where(allowed, 0.0, masked_score).astype(jnp.bfloat16)
    same = (row_iota == lax.broadcasted_iota(jnp.int32, (rows, rows), 1)).astype(jnp.bfloat16)
    for i in range(QPER):
        eye[pl.ds(i * rows, rows)] = same.astype(jnp.bfloat16)
    ones[...] = jnp.ones_like(ones)
    for offset in range(1, COLUMNS):
        for copy in to_column(offset):
            copy.start()
    learn(0)
    tell(1)

    def piece(i, group):
        c, layer = i // LAYERS, i % LAYERS
        first, count = GROUPS[group]
        last = group == len(GROUPS) - 1
        keys = pl.ds(first * rows, count * rows)
        wide_q = jnp.concatenate([qs[c, layer], eye[...]], axis=1)
        wide_k = jnp.concatenate([held[0, c, keys], bias[keys]], axis=1)
        scores = lax.dot_general(
            wide_q, wide_k, (((1,), (1,)), ((), ())), preferred_element_type=jnp.float32
        )
        fresh = jnp.max(scores, axis=1, keepdims=True)
        if first > 0:
            old = top[c, layer]
            fresh = jnp.maximum(old, fresh)
            shrink = jnp.exp2((old - fresh) * exponent_scale)
            fresh = fresh[:, :1]
        weights = jnp.exp2((scores - fresh) * exponent_scale)
        wide_v = jnp.concatenate([held[1, c, keys], ones[pl.ds(0, count * rows)]], axis=1)
        product = jnp.dot(weights.astype(jnp.bfloat16), wide_v, preferred_element_type=jnp.float32)
        summed, counted = product[:, :HD], product[:, HD:]
        if first > 0:
            summed = acc[c, layer] * shrink + summed
            counted = total[c, layer] * shrink + counted
        if last:
            done = (summed / counted).astype(o_ref.dtype)
            for q in range(QPER):
                h = c * QPER + q
                place = h * HD if isinstance(h, int) else pl.multiple_of(h * HD, HD)
                o_ref[layer, :, pl.ds(place, HD)] = done[q * rows:(q + 1) * rows]
        else:
            top[c, layer] = jnp.broadcast_to(fresh, (QPER * rows, HD))
            acc[c, layer] = summed
            total[c, layer] = counted

    def handle(n, forward=True):
        hop(n).wait_recv()
        if forward:
            hop(n + parts).start()

    def loop(count, body):
        def step(i, carry):
            body(i)
            return carry

        lax.fori_loop(0, count, step, 0)

    half = places // 2
    detour = half - FORWARD

    def send_back(k):
        for copy in to_place(-k, half + k):
            copy.start()

    def send_ahead(k):
        for copy in to_place(k, k):
            copy.start()

    def send_both(k):
        send_back(k)
        send_ahead(k)

    def to_stop(j):
        there = lax.rem(place + FORWARD + 1 + j, places)
        here = pl.ds(pl.multiple_of(there * unit, unit), unit)
        return [
            pltpu.make_async_remote_copy(
                src_ref=src,
                dst_ref=dst,
                send_sem=stop_send.at[part, j],
                recv_sem=stop_recv.at[part, j],
                device_id={"seq": at_place(-STOP)},
                device_id_type=MESH,
            )
            for part, (src, dst) in enumerate(
                (
                    (along.at[here], stopped.at[pl.ds(pl.multiple_of(j * unit, unit), unit)]),
                    (tag_along.at[there], tag_stopped.at[j]),
                )
            )
        ]

    def from_stop(j):
        landing = FORWARD + 1 + j
        return [
            pltpu.make_async_remote_copy(
                src_ref=src,
                dst_ref=dst,
                send_sem=along_send.at[part, landing],
                recv_sem=along_recv.at[part, landing],
                device_id={"seq": at_place(STOP + landing - places)},
                device_id_type=MESH,
            )
            for part, (src, dst) in enumerate(
                (
                    (
                        stopped.at[pl.ds(pl.multiple_of(j * unit, unit), unit)],
                        landed.at[pl.ds(pl.multiple_of(landing * unit, unit), unit)],
                    ),
                    (tag_stopped.at[j], tag_landed.at[landing]),
                )
            )
        ]

    learn(1)
    tell(2)
    loop(parts, handle)
    for offset in range(1, COLUMNS):
        for copy in to_column(offset):
            copy.wait_recv()
    row = iota((seq_count * PAGE, seq_count * PAGE), 0)
    regroup = (row % unit) // PAGE * lines + row // unit * PAGE + row % PAGE
    along[...] = jnp.dot(
        one_hot(regroup == iota((seq_count * PAGE, seq_count * PAGE), 1)),
        across[...],
        preferred_element_type=jnp.float32,
    ).astype(jnp.bfloat16)
    tag_rows = jnp.zeros((HD, seq_count), jnp.float32)
    for x in range(COLUMNS):
        mask = (iota((HD, seq_count), 0) % unit) // PAGE == x
        tag_rows = jnp.where(mask, jnp.broadcast_to(tag_across[x], (HD, seq_count)), tag_rows)
    choose = iota((places, seq_count), 1) == column * places + iota((places, seq_count), 0)
    tag_table = lax.dot_general(
        one_hot(choose),
        tag_rows.astype(jnp.bfloat16),
        (((1,), (1,)), ((), ())),
        preferred_element_type=jnp.float32,
    )
    for z in range(places):
        tag_along[z] = tag_table[z:z + 1]
    landed[pl.ds(0, unit)] = along[pl.ds(pl.multiple_of(place * unit, unit), unit)]
    tag_landed[0] = tag_along[place]
    loop(NEAR, lambda i: send_both(i + 1))
    learn(2)
    tell(3)
    for j in range(detour):
        for copy in to_stop(j):
            copy.start()
    loop(STOP - NEAR, lambda i: send_both(NEAR + 1 + i))

    for load in loads[parts + 3:]:
        load.wait()
    pieces = kv_local * LAYERS
    last_chunks = (REACH - 1) * parts

    def beside(group):
        first_chunk = (GROUPS[group][0] + 1) * parts

        def step(i):
            handle(first_chunk + i)
            piece(i, group)

        loop(pieces, step)
        for n in range(first_chunk + pieces, first_chunk + 2 * parts):
            handle(n)

    beside(0)
    learn(3)
    loop(half - 1 - STOP, lambda i: send_back(STOP + 1 + i))
    beside(1)
    loop(FORWARD - STOP, lambda i: send_ahead(STOP + 1 + i))
    for j in range(detour):
        for copy in to_stop(j):
            copy.wait_recv()
        for copy in from_stop(j):
            copy.start()
    beside(2)

    def wait_sent(landing):
        for copy in to_place(1, landing):
            copy.wait_send()

    settled = 4 * parts
    loop(settled + parts, lambda n: hop(n).wait_send())
    for offset in range(1, COLUMNS):
        for copy in to_column(offset):
            copy.wait_send()
    for j in range(detour):
        for copy in to_stop(j):
            copy.wait_send()
    loop(STOP, lambda i: wait_sent(1 + i))
    loop(STOP, lambda i: wait_sent(half + 1 + i))
    for n in range(last_chunks, last_chunks + 2):
        handle(n, False)

    def last_group(i):
        @pl.when(i < 2)
        def _():
            handle(last_chunks + 2 + i, False)

        piece(i, 3)

    loop(pieces, last_group)

    def wait_pages(i):
        for copy in to_place(1, i + 1):
            copy.wait_recv()

    loop(places - 1, wait_pages)
    came = jnp.concatenate([tag_landed[z] for z in range(places)], axis=0)
    spread = jnp.dot(
        one_hot(iota((seq_count * PAGE, places), 0) // unit == iota((seq_count * PAGE, places), 1)),
        came.astype(jnp.bfloat16),
        preferred_element_type=jnp.float32,
    )
    here = iota((seq_count * PAGE, HD), 0) % unit == iota((seq_count * PAGE, HD), 1)
    tag_column = jnp.sum(jnp.where(here, spread, 0.0), axis=1, keepdims=True)
    line_column = (iota((seq_count * PAGE, 1), 0) % PAGE).astype(jnp.float32)
    lands = (tag_column - 1.0) * PAGE + line_column
    slot_lines = page_ref.shape[0]
    put = iota((seq_count * PAGE, slot_lines), 1).astype(jnp.float32) == lands
    page_ref[...] = lax.dot_general(
        one_hot(put), landed[...], (((0,), (0,)), ((), ())), preferred_element_type=jnp.float32
    ).astype(page_ref.dtype)

    loop(last_chunks - settled, lambda n: hop(settled + parts + n).wait_send())
    loop(half - 1 - STOP, lambda i: wait_sent(half + STOP + 1 + i))
    loop(half - STOP, lambda i: wait_sent(STOP + 1 + i))


def shards(queries, keys, values, lengths, page_owner, page_slot):
    rows = keys.shape[0]
    kv_local = keys.shape[1] // HD
    seq_count = lax.axis_size("seq")
    width = queries.shape[2]
    wide = QPER * rows
    pages_dev = rows // PAGE
    slots = pages_dev * kv_local
    places = seq_count // COLUMNS
    lines = seq_count * PAGE
    detour = places // 2 - FORWARD
    attended, pages = pl.pallas_call(
        functools.partial(ring_attention, seq_count),
        name="ring_attention",
        out_shape=(
            jax.ShapeDtypeStruct((LAYERS, rows, width), jnp.bfloat16),
            jax.ShapeDtypeStruct((slots * PAGE, 2 * HD), jnp.bfloat16),
        ),
        in_specs=[pl.BlockSpec(memory_space=pltpu.HBM)] * 6,
        out_specs=(pl.BlockSpec(memory_space=pltpu.VMEM), pl.BlockSpec(memory_space=pltpu.VMEM)),
        scratch_shapes=[
            pltpu.VMEM((1, lengths.shape[0]), jnp.int32),
            pltpu.VMEM((kv_local, pages_dev), jnp.int32),
            pltpu.VMEM((kv_local, pages_dev), jnp.int32),
            pltpu.SemaphoreType.DMA((2 * kv_local + 3 + kv_local * LAYERS * QPER,)),
            pltpu.VMEM((kv_local, LAYERS, wide, HD), jnp.bfloat16),
            pltpu.VMEM((2, kv_local, (REACH + 1) * rows, HD), jnp.bfloat16),
            pltpu.VMEM(((REACH + 1) * rows, rows), jnp.bfloat16),
            pltpu.VMEM((wide, rows), jnp.bfloat16),
            pltpu.VMEM((max(count for _, count in GROUPS) * rows, HD), jnp.bfloat16),
            pltpu.VMEM((kv_local, LAYERS, wide, HD), jnp.float32),
            pltpu.VMEM((kv_local, LAYERS, wide, HD), jnp.float32),
            pltpu.VMEM((kv_local, LAYERS, wide, HD), jnp.float32),
            pltpu.SemaphoreType.DMA((REACH * kv_local * 2,)),
            pltpu.SemaphoreType.DMA((REACH * kv_local * 2,)),
            pltpu.VMEM((lines, 2 * HD), jnp.bfloat16),
            pltpu.VMEM((lines, 2 * HD), jnp.bfloat16),
            pltpu.VMEM((lines, 2 * HD), jnp.bfloat16),
            pltpu.VMEM((lines, 2 * HD), jnp.bfloat16),
            pltpu.VMEM((COLUMNS, 1, seq_count), jnp.float32),
            pltpu.VMEM((places, 1, HD), jnp.float32),
            pltpu.VMEM((places, 1, HD), jnp.float32),
            pltpu.VMEM((detour * COLUMNS * PAGE, 2 * HD), jnp.bfloat16),
            pltpu.VMEM((detour, 1, HD), jnp.float32),
            pltpu.SemaphoreType.DMA((2, COLUMNS)),
            pltpu.SemaphoreType.DMA((2, COLUMNS)),
            pltpu.SemaphoreType.DMA((2, places)),
            pltpu.SemaphoreType.DMA((2, places)),
            pltpu.SemaphoreType.DMA((2, detour)),
            pltpu.SemaphoreType.DMA((2, detour)),
            pltpu.SemaphoreType.REGULAR((4,)),
            pltpu.SemaphoreType.REGULAR((4,)),
        ],
        compiler_params=pltpu.CompilerParams(
            collective_id=0, has_side_effects=True, vmem_limit_bytes=28 * 1024 * 1024
        ),
    )(
        *(
            pltpu.with_memory_space_constraint(x, pltpu.HBM)
            for x in (
                queries.transpose(1, 0, 2), keys, values, lengths.reshape(1, -1),
                page_owner.transpose(1, 0), page_slot.transpose(1, 0),
            )
        )
    )
    return (attended.transpose(1, 0, 2), pages.reshape(slots, PAGE, 2 * HD))


def solution(mesh):
    placed = (
        P(("group", "seq"), None, "head"),
        P(("group", "seq"), "head"),
        P(("group", "seq"), "head"),
        P("group"),
        P(("group", "seq"), "head"),
        P(("group", "seq"), "head"),
    )
    return jax.shard_map(
        shards,
        mesh=mesh,
        in_specs=placed,
        out_specs=(P(("group", "seq"), None, "head"), P(("group", "seq", "head"), None, None)),
        check_vma=False,
    )
```

```python
import functools
import math

import jax
import jax.numpy as jnp
from jax import lax
from jax.experimental import pallas as pl
from jax.experimental.pallas import tpu as pltpu
from jax.sharding import PartitionSpec as P

LAYERS = 3
QPER = 5
HD = 128
PAGE = 4
REACH = 8
GROUPS = ((0, 2), (2, 2), (4, 2), (6, 3))
COLUMNS = 4
STOP = 8
FORWARD = 12
NEAR = 4
LATEST = 10
MESH = pl.DeviceIdType.MESH

masked_score = -16384.0
exponent_scale = math.log2(math.e) / math.sqrt(HD)


def ring_attention(
    seq_count, q_hbm, k_hbm, v_hbm, len_hbm, owner_hbm, slot_hbm, o_ref, page_ref,
    len_ref, owner_ref, slot_ref, load_sem, qs, held, bias, eye, ones, top, acc, total, send_sem, recv_sem,
    picked, across, along, landed, tag_across, tag_along, tag_landed,
    stopped, tag_stopped,
    across_send, across_recv, along_send, along_recv, stop_send, stop_recv, from_right, from_left,
):
    rows = k_hbm.shape[0]
    kv_local = held.shape[1]
    parts = 2 * kv_local
    mine = lax.axis_index("seq")
    right = lax.rem(mine + 1, seq_count)
    left = lax.rem(mine + seq_count - 1, seq_count)

    places = seq_count // COLUMNS
    column, place = mine // places, lax.rem(mine, places)

    def at_place(offset):
        return column * places + lax.rem(place + places + offset, places)

    def at_column(offset):
        return lax.rem(column + COLUMNS + offset, COLUMNS) * places + place

    def signal(sem, device):
        pl.semaphore_signal(sem, inc=1, device_id={"seq": device}, device_id_type=MESH)

    own = pl.ds(0, rows)
    pairs = [
        (ref.at[:, pl.ds(c * HD, HD)], held.at[part, c, own])
        for c in range(kv_local)
        for part, ref in enumerate((k_hbm, v_hbm))
    ]
    pairs += [(owner_hbm, owner_ref), (slot_hbm, slot_ref), (len_hbm, len_ref)]
    pairs += [
        (
            q_hbm.at[layer, :, pl.ds((c * QPER + i) * HD, HD)],
            qs.at[c, layer, pl.ds(i * rows, rows)],
        )
        for c in range(kv_local)
        for layer in range(LAYERS)
        for i in range(QPER)
    ]
    loads = [
        pltpu.make_async_copy(src, dst, load_sem.at[n]) for n, (src, dst) in enumerate(pairs)
    ]
    for load in loads:
        load.start()

    barrier = pltpu.get_barrier_semaphore()
    signal(barrier, left)
    signal(barrier, at_place(1))
    signal(barrier, at_place(-1))
    for offset in range(1, COLUMNS):
        signal(barrier, at_column(offset))
    pl.semaphore_wait(barrier, COLUMNS + 2)
    def tell(level):
        signal(from_right.at[level], at_place(-(1 << level)))
        signal(from_left.at[level], at_place(1 << level))

    def learn(level):
        pl.semaphore_wait(from_right.at[level], 1)
        pl.semaphore_wait(from_left.at[level], 1)

    def hop(n):
        slot = n // parts
        c, part = (n % parts) // 2, n % 2
        return pltpu.make_async_remote_copy(
            src_ref=held.at[part, c, pl.ds(pl.multiple_of(slot * rows, rows), rows)],
            dst_ref=held.at[part, c, pl.ds(pl.multiple_of((slot + 1) * rows, rows), rows)],
            send_sem=send_sem.at[n],
            recv_sem=recv_sem.at[n],
            device_id={"seq": right},
            device_id_type=MESH,
        )

    for n in range(parts):
        loads[n].wait()
        hop(n).start()
    tell(0)
    for load in loads[parts:parts + 3]:
        load.wait()

    lines = places * PAGE
    unit = COLUMNS * PAGE

    def iota(shape, axis):
        return lax.broadcasted_iota(jnp.int32, shape, axis)

    pages_dev = rows // PAGE
    widen = (iota((pages_dev, rows), 0) == iota((pages_dev, rows), 1) // PAGE).astype(jnp.bfloat16)

    def per_token(ref):
        wide = jnp.dot(
            ref[...].astype(jnp.float32).astype(jnp.bfloat16), widen, preferred_element_type=jnp.float32
        )
        return jnp.concatenate([wide[c:c + 1] for c in range(kv_local)], axis=1)

    owner_row = per_token(owner_ref)
    slot_row = per_token(slot_ref) + 1.0
    line_row = (iota((1, kv_local * rows), 1) % PAGE).astype(jnp.float32)
    goes = iota((seq_count * PAGE, kv_local * rows), 0).astype(jnp.float32) == owner_row * PAGE + line_row
    source = jnp.concatenate(
        [
            jnp.concatenate([held[0, c, own], held[1, c, own]], axis=1)
            for c in range(kv_local)
        ],
        axis=0,
    )

    def one_hot(mask):
        return jnp.where(mask, 1.0, 0.0).astype(jnp.bfloat16)

    picked[...] = jnp.dot(one_hot(goes), source, preferred_element_type=jnp.float32).astype(jnp.bfloat16)
    owned = (iota((seq_count, kv_local * rows), 0).astype(jnp.float32) == owner_row) & (
        jnp.broadcast_to(line_row, (seq_count, kv_local * rows)) == 0.0
    )
    tags = lax.dot_general(
        jnp.broadcast_to(slot_row, (8, kv_local * rows)).astype(jnp.bfloat16),
        one_hot(owned),
        (((1,), (1,)), ((), ())),
        preferred_element_type=jnp.float32,
    )
    tag_across[column] = tags[:1]
    own_lines = pl.ds(pl.multiple_of(column * lines, lines), lines)
    across[own_lines] = picked[own_lines]

    def to_column(offset):
        device = at_column(offset)
        first = pl.multiple_of((device // places) * lines, lines)
        return [
            pltpu.make_async_remote_copy(
                src_ref=src,
                dst_ref=dst,
                send_sem=across_send.at[part, offset],
                recv_sem=across_recv.at[part, offset],
                device_id={"seq": device},
                device_id_type=MESH,
            )
            for part, (src, dst) in enumerate(
                (
                    (picked.at[pl.ds(first, lines)], across.at[own_lines]),
                    (tag_across.at[column], tag_across.at[column]),
                )
            )
        ]

    def to_place(offset, landing):
        device = at_place(offset)
        there = lax.rem(device, places)
        return [
            pltpu.make_async_remote_copy(
                src_ref=src,
                dst_ref=dst,
                send_sem=along_send.at[part, landing],
                recv_sem=along_recv.at[part, landing],
                device_id={"seq": device},
                device_id_type=MESH,
            )
            for part, (src, dst) in enumerate(
                (
                    (
                        along.at[pl.ds(pl.multiple_of(there * unit, unit), unit)],
                        landed.at[pl.ds(pl.multiple_of(landing * unit, unit), unit)],
                    ),
                    (tag_along.at[there], tag_landed.at[landing]),
                )
            )
        ]

    reqs = len_ref.shape[1]
    lengths = len_ref[...].astype(jnp.float32)
    before = lax.broadcasted_iota(jnp.int32, (reqs, reqs), 1) < lax.broadcasted_iota(
        jnp.int32, (reqs, reqs), 0
    )
    starts = jnp.sum(
        jnp.where(before, jnp.broadcast_to(lengths, (reqs, reqs)), 0.0), axis=1, keepdims=True
    )
    query_pos = (mine * rows + lax.broadcasted_iota(jnp.int32, (reqs, rows), 1)).astype(jnp.float32)
    began = jnp.max(jnp.where(starts <= query_pos, starts, 0.0), axis=0, keepdims=True)
    token = (mine * rows + lax.broadcasted_iota(jnp.int32, (rows, rows), 1)).astype(jnp.float32)
    row_iota = lax.broadcasted_iota(jnp.int32, (rows, rows), 0)
    for d in range(REACH + 1):
        key_pos = ((mine - d) * rows + row_iota).astype(jnp.float32)
        allowed = (key_pos >= began) & (key_pos <= token)
        bias[pl.ds(d * rows, rows)] = jnp.where(allowed, 0.0, masked_score).astype(jnp.bfloat16)
    same = (row_iota == lax.broadcasted_iota(jnp.int32, (rows, rows), 1)).astype(jnp.bfloat16)
    for i in range(QPER):
        eye[pl.ds(i * rows, rows)] = same.astype(jnp.bfloat16)
    ones[...] = jnp.ones_like(ones)
    for offset in range(1, COLUMNS):
        for copy in to_column(offset):
            copy.start()
    learn(0)
    tell(1)

    def piece(i, group):
        c, layer = i // LAYERS, i % LAYERS
        first, count = GROUPS[group]
        last = group == len(GROUPS) - 1
        keys = pl.ds(first * rows, count * rows)
        wide_q = jnp.concatenate([qs[c, layer], eye[...]], axis=1)
        wide_k = jnp.concatenate([held[0, c, keys], bias[keys]], axis=1)
        scores = lax.dot_general(
            wide_q, wide_k, (((1,), (1,)), ((), ())), preferred_element_type=jnp.float32
        )
        fresh = jnp.max(scores, axis=1, keepdims=True)
        if first > 0:
            old = top[c, layer]
            fresh = jnp.maximum(old, fresh)
            shrink = jnp.exp2((old - fresh) * exponent_scale)
            fresh = fresh[:, :1]
        weights = jnp.exp2((scores - fresh) * exponent_scale)
        wide_v = jnp.concatenate([held[1, c, keys], ones[pl.ds(0, count * rows)]], axis=1)
        product = jnp.dot(weights.astype(jnp.bfloat16), wide_v, preferred_element_type=jnp.float32)
        summed, counted = product[:, :HD], product[:, HD:]
        if first > 0:
            summed = acc[c, layer] * shrink + summed
            counted = total[c, layer] * shrink + counted
        if last:
            done = (summed / counted).astype(o_ref.dtype)
            for q in range(QPER):
                h = c * QPER + q
                place = h * HD if isinstance(h, int) else pl.multiple_of(h * HD, HD)
                o_ref[layer, :, pl.ds(place, HD)] = done[q * rows:(q + 1) * rows]
        else:
            top[c, layer] = jnp.broadcast_to(fresh, (QPER * rows, HD))
            acc[c, layer] = summed
            total[c, layer] = counted

    def handle(n, forward=True):
        hop(n).wait_recv()
        if forward:
            hop(n + parts).start()

    def loop(count, body):
        def step(i, carry):
            body(i)
            return carry

        lax.fori_loop(0, count, step, 0)

    half = places // 2
    detour = half - FORWARD

    def send_back(k):
        for copy in to_place(-k, half + k):
            copy.start()

    def send_ahead(k):
        for copy in to_place(k, k):
            copy.start()

    def send_both(k):
        send_back(k)
        send_ahead(k)

    def to_stop(j):
        there = lax.rem(place + FORWARD + 1 + j, places)
        here = pl.ds(pl.multiple_of(there * unit, unit), unit)
        return [
            pltpu.make_async_remote_copy(
                src_ref=src,
                dst_ref=dst,
                send_sem=stop_send.at[part, j],
                recv_sem=stop_recv.at[part, j],
                device_id={"seq": at_place(-STOP)},
                device_id_type=MESH,
            )
            for part, (src, dst) in enumerate(
                (
                    (along.at[here], stopped.at[pl.ds(pl.multiple_of(j * unit, unit), unit)]),
                    (tag_along.at[there], tag_stopped.at[j]),
                )
            )
        ]

    def from_stop(j):
        landing = FORWARD + 1 + j
        return [
            pltpu.make_async_remote_copy(
                src_ref=src,
                dst_ref=dst,
                send_sem=along_send.at[part, landing],
                recv_sem=along_recv.at[part, landing],
                device_id={"seq": at_place(STOP + landing - places)},
                device_id_type=MESH,
            )
            for part, (src, dst) in enumerate(
                (
                    (
                        stopped.at[pl.ds(pl.multiple_of(j * unit, unit), unit)],
                        landed.at[pl.ds(pl.multiple_of(landing * unit, unit), unit)],
                    ),
                    (tag_stopped.at[j], tag_landed.at[landing]),
                )
            )
        ]

    learn(1)
    tell(2)
    loop(parts, handle)
    for offset in range(1, COLUMNS):
        for copy in to_column(offset):
            copy.wait_recv()
    row = iota((seq_count * PAGE, seq_count * PAGE), 0)
    regroup = (row % unit) // PAGE * lines + row // unit * PAGE + row % PAGE
    along[...] = jnp.dot(
        one_hot(regroup == iota((seq_count * PAGE, seq_count * PAGE), 1)),
        across[...],
        preferred_element_type=jnp.float32,
    ).astype(jnp.bfloat16)
    tag_rows = jnp.zeros((HD, seq_count), jnp.float32)
    for x in range(COLUMNS):
        mask = (iota((HD, seq_count), 0) % unit) // PAGE == x
        tag_rows = jnp.where(mask, jnp.broadcast_to(tag_across[x], (HD, seq_count)), tag_rows)
    choose = iota((places, seq_count), 1) == column * places + iota((places, seq_count), 0)
    tag_table = lax.dot_general(
        one_hot(choose),
        tag_rows.astype(jnp.bfloat16),
        (((1,), (1,)), ((), ())),
        preferred_element_type=jnp.float32,
    )
    for z in range(places):
        tag_along[z] = tag_table[z:z + 1]
    landed[pl.ds(0, unit)] = along[pl.ds(pl.multiple_of(place * unit, unit), unit)]
    tag_landed[0] = tag_along[place]
    loop(NEAR, lambda i: send_both(i + 1))
    learn(2)
    tell(3)
    for j in range(detour):
        for copy in to_stop(j):
            copy.start()
    loop(STOP - NEAR, lambda i: send_both(NEAR + 1 + i))

    for load in loads[parts + 3:]:
        load.wait()
    pieces = kv_local * LAYERS
    last_chunks = (REACH - 1) * parts

    def beside(group, then=None):
        first_chunk = (GROUPS[group][0] + 1) * parts

        def step(i):
            handle(first_chunk + i)
            piece(i, group)

        loop(pieces, step)
        if then is not None:
            then()
        for n in range(first_chunk + pieces, first_chunk + 2 * parts):
            handle(n)

    beside(0)
    learn(3)
    loop(half - 1 - STOP, lambda i: send_back(STOP + 1 + i))
    beside(1)
    loop(FORWARD - LATEST, lambda i: send_ahead(FORWARD - i))
    for j in range(detour):
        for copy in to_stop(j):
            copy.wait_recv()
        for copy in from_stop(j):
            copy.start()
    beside(2, lambda: loop(LATEST - STOP, lambda i: send_ahead(LATEST - i)))

    def wait_sent(landing):
        for copy in to_place(1, landing):
            copy.wait_send()

    settled = 4 * parts
    loop(settled + parts, lambda n: hop(n).wait_send())
    for offset in range(1, COLUMNS):
        for copy in to_column(offset):
            copy.wait_send()
    for j in range(detour):
        for copy in to_stop(j):
            copy.wait_send()
    loop(STOP, lambda i: wait_sent(1 + i))
    loop(STOP, lambda i: wait_sent(half + 1 + i))
    for n in range(last_chunks, last_chunks + 2):
        handle(n, False)

    def last_group(i):
        @pl.when(i < 2)
        def _():
            handle(last_chunks + 2 + i, False)

        piece(i, 3)

    loop(pieces, last_group)

    def wait_pages(i):
        for copy in to_place(1, i + 1):
            copy.wait_recv()

    loop(places - 1, wait_pages)
    came = jnp.concatenate([tag_landed[z] for z in range(places)], axis=0)
    spread = jnp.dot(
        one_hot(iota((seq_count * PAGE, places), 0) // unit == iota((seq_count * PAGE, places), 1)),
        came.astype(jnp.bfloat16),
        preferred_element_type=jnp.float32,
    )
    here = iota((seq_count * PAGE, HD), 0) % unit == iota((seq_count * PAGE, HD), 1)
    tag_column = jnp.sum(jnp.where(here, spread, 0.0), axis=1, keepdims=True)
    line_column = (iota((seq_count * PAGE, 1), 0) % PAGE).astype(jnp.float32)
    lands = (tag_column - 1.0) * PAGE + line_column
    slot_lines = page_ref.shape[0]
    put = iota((seq_count * PAGE, slot_lines), 1).astype(jnp.float32) == lands
    page_ref[...] = lax.dot_general(
        one_hot(put), landed[...], (((0,), (0,)), ((), ())), preferred_element_type=jnp.float32
    ).astype(page_ref.dtype)

    loop(last_chunks - settled, lambda n: hop(settled + parts + n).wait_send())
    loop(half - 1 - STOP, lambda i: wait_sent(half + STOP + 1 + i))
    loop(half - STOP, lambda i: wait_sent(STOP + 1 + i))


def shards(queries, keys, values, lengths, page_owner, page_slot):
    rows = keys.shape[0]
    kv_local = keys.shape[1] // HD
    seq_count = lax.axis_size("seq")
    width = queries.shape[2]
    wide = QPER * rows
    pages_dev = rows // PAGE
    slots = pages_dev * kv_local
    places = seq_count // COLUMNS
    lines = seq_count * PAGE
    detour = places // 2 - FORWARD
    attended, pages = pl.pallas_call(
        functools.partial(ring_attention, seq_count),
        name="ring_attention",
        out_shape=(
            jax.ShapeDtypeStruct((LAYERS, rows, width), jnp.bfloat16),
            jax.ShapeDtypeStruct((slots * PAGE, 2 * HD), jnp.bfloat16),
        ),
        in_specs=[pl.BlockSpec(memory_space=pltpu.HBM)] * 6,
        out_specs=(pl.BlockSpec(memory_space=pltpu.VMEM), pl.BlockSpec(memory_space=pltpu.VMEM)),
        scratch_shapes=[
            pltpu.VMEM((1, lengths.shape[0]), jnp.int32),
            pltpu.VMEM((kv_local, pages_dev), jnp.int32),
            pltpu.VMEM((kv_local, pages_dev), jnp.int32),
            pltpu.SemaphoreType.DMA((2 * kv_local + 3 + kv_local * LAYERS * QPER,)),
            pltpu.VMEM((kv_local, LAYERS, wide, HD), jnp.bfloat16),
            pltpu.VMEM((2, kv_local, (REACH + 1) * rows, HD), jnp.bfloat16),
            pltpu.VMEM(((REACH + 1) * rows, rows), jnp.bfloat16),
            pltpu.VMEM((wide, rows), jnp.bfloat16),
            pltpu.VMEM((max(count for _, count in GROUPS) * rows, HD), jnp.bfloat16),
            pltpu.VMEM((kv_local, LAYERS, wide, HD), jnp.float32),
            pltpu.VMEM((kv_local, LAYERS, wide, HD), jnp.float32),
            pltpu.VMEM((kv_local, LAYERS, wide, HD), jnp.float32),
            pltpu.SemaphoreType.DMA((REACH * kv_local * 2,)),
            pltpu.SemaphoreType.DMA((REACH * kv_local * 2,)),
            pltpu.VMEM((lines, 2 * HD), jnp.bfloat16),
            pltpu.VMEM((lines, 2 * HD), jnp.bfloat16),
            pltpu.VMEM((lines, 2 * HD), jnp.bfloat16),
            pltpu.VMEM((lines, 2 * HD), jnp.bfloat16),
            pltpu.VMEM((COLUMNS, 1, seq_count), jnp.float32),
            pltpu.VMEM((places, 1, HD), jnp.float32),
            pltpu.VMEM((places, 1, HD), jnp.float32),
            pltpu.VMEM((detour * COLUMNS * PAGE, 2 * HD), jnp.bfloat16),
            pltpu.VMEM((detour, 1, HD), jnp.float32),
            pltpu.SemaphoreType.DMA((2, COLUMNS)),
            pltpu.SemaphoreType.DMA((2, COLUMNS)),
            pltpu.SemaphoreType.DMA((2, places)),
            pltpu.SemaphoreType.DMA((2, places)),
            pltpu.SemaphoreType.DMA((2, detour)),
            pltpu.SemaphoreType.DMA((2, detour)),
            pltpu.SemaphoreType.REGULAR((4,)),
            pltpu.SemaphoreType.REGULAR((4,)),
        ],
        compiler_params=pltpu.CompilerParams(
            collective_id=0, has_side_effects=True, vmem_limit_bytes=28 * 1024 * 1024
        ),
    )(
        *(
            pltpu.with_memory_space_constraint(x, pltpu.HBM)
            for x in (
                queries.transpose(1, 0, 2), keys, values, lengths.reshape(1, -1),
                page_owner.transpose(1, 0), page_slot.transpose(1, 0),
            )
        )
    )
    return (attended.transpose(1, 0, 2), pages.reshape(slots, PAGE, 2 * HD))


def solution(mesh):
    placed = (
        P(("group", "seq"), None, "head"),
        P(("group", "seq"), "head"),
        P(("group", "seq"), "head"),
        P("group"),
        P(("group", "seq"), "head"),
        P(("group", "seq"), "head"),
    )
    return jax.shard_map(
        shards,
        mesh=mesh,
        in_specs=placed,
        out_specs=(P(("group", "seq"), None, "head"), P(("group", "seq", "head"), None, None)),
        check_vma=False,
    )
```
